256 devices in a mesh: dp: 8 (over z_lo, core), expert: 32 (over y, x, z_hi).
Axes of the slice: x: 4, y: 4, z: 8 (z_hi: 2, z_lo: 4; z = z_hi * 4 + z_lo), core: 2. Of those that a mesh axis runs over, the one named last changes fastest.
Arguments:
- tokens: bfloat16 [32768, 3584], P(('dp', 'expert')), may hold values from -6 to 6
- cotangent: bfloat16 [32768, 3584], P(('dp', 'expert')), may hold values from -6 to 6
- gates: float32 [32768, 1], P(('dp', 'expert')), may hold values from 0.1 to 1
- routes: int32 [32768, 1], P(('dp', 'expert')), may hold values from 0 to 31; in each aligned block of 128 rows (0 to 127, 128 to 255, ...) at most 5 rows name the same one
- w_up: bfloat16 [32, 3584, 1024], P('expert', None, 'dp'), may hold values from -0.09375 to 0.09375
- w_down: bfloat16 [32, 1024, 3584], P('expert', 'dp'), may hold values from -0.1875 to 0.1875
- m_up: bfloat16 [32, 3584, 1024], P('expert', None, 'dp'), may hold values from -3 to 3
- v_up: bfloat16 [32, 3584, 1024], P('expert', None, 'dp'), may hold values from 0.099609375 to 1
- m_down: bfloat16 [32, 1024, 3584], P('expert', 'dp'), may hold values from -3 to 3
- v_down: bfloat16 [32, 1024, 3584], P('expert', 'dp'), may hold values from 0.099609375 to 1
- leaving: int32 [1], replicated, may hold values from 0 to 31
- tile_owner: int32 [32], replicated, may hold values from 0 to 31, each once
Outputs:
- update_up: bfloat16 [32, 3584, 1024], P('expert', None, 'dp')
- update_down: bfloat16 [32, 1024, 3584], P('expert', 'dp')
- adopted_up: bfloat16 [32, 112, 1024], P('expert', None, 'dp')
- adopted_down: bfloat16 [32, 112, 1024], P('expert', None, 'dp')
The draws below stay inside these ranges and needn't reach their ends.
Inputs may be any that keep to these rules, and one draw needn't show every extreme that they name: `routes`: each row names one expert; within the 128 rows of one device no expert is named more than 5 times, a bound that some block reaches in some devices. `tile_owner`: A permutation of the 32 device indices of the expert axis.
All inputs are finite; a program needn't handle non-finite values.
Results may differ from the reference program's by a relative error of at most 0.0041.
Values may be sent and summed in bfloat16 or wider, within the bound.
A program may use at most 128 MiB of HBM per device.

```python
import math
import jax
import jax.numpy as jnp
import numpy as np
from jax import lax

D = 3584
FF = 1024
TOK_DEV = 128
TOPK = 1
EXPERTS = 32
TOKENS = 32768
CAP = 5
DEVICES = 256


def level_of(key, shape, shards, smallest, largest):
    factor_of, own = 1.0, jax.random.fold_in(key, 6)
    for position, shards_of in shards:
        heights = jnp.exp(jax.random.uniform(jax.random.fold_in(own, position), (shards_of,), jnp.float32, smallest / len(shards), largest / len(shards)))
        factor_of = factor_of * jnp.repeat(heights, shape[position] // shards_of).reshape([-1 if axis == position else 1 for axis in range(len(shape))])
    return factor_of


def deal_out(stream_key, own, number, rows, count, top, reach, skew):
    order = jax.random.permutation(stream_key, count)
    packed, ordinary = portions_of(count, rows * top, reach, skew, True), portions_of(count, rows * top, reach, skew, False)
    places = jnp.arange(count)

    def named(sizes, rotation):
        used = int((sizes > 0).sum())
        fixed = max(1, used // 4)
        shifted = fixed + (places - fixed + rotation * (used - fixed)) % max(1, count - fixed)
        return jnp.zeros((count,), jnp.int32).at[order[jnp.where(places < fixed, places, shifted)]].set(jnp.asarray(sizes, jnp.int32))

    sizes = jnp.where(number % 4 == 0, named(packed, number // 4), named(ordinary, number - number // 4 - 1))
    mixed = jax.random.permutation(jax.random.fold_in(own, 3), count)
    giver, receiver = mixed[0:count // 2 * 2:2], mixed[1:count // 2 * 2:2]
    room = jnp.minimum(sizes[giver] - 1, reach - sizes[receiver]) // 2
    room = jnp.where((giver == order[0]) | (receiver == order[0]) | (sizes[receiver] == 0), 0, jnp.maximum(room, 0))
    shifted = jax.random.randint(jax.random.fold_in(own, 4), (count // 2,), 0, 1 << 20) % (room + 1)
    sizes = sizes.at[giver].add(-shifted).at[receiver].add(shifted)
    labels = jnp.searchsorted(jnp.cumsum(sizes), jnp.arange(rows * top), side="right").astype(jnp.int32)
    listing = labels.reshape(top, rows).T
    listing = listing[jax.random.permutation(jax.random.fold_in(own, 1), rows)]
    rotation = jax.random.randint(jax.random.fold_in(own, 2), (rows, 1), 0, top)
    return jnp.take_along_axis(listing, (jnp.arange(top)[None, :] + rotation) % top, axis=1)


def portions_of(number_of, total, bound, lean, full):
    weights = [(1 << 20) // math.isqrt(grade ** lean) + 1 for grade in range(1, number_of + 1)]
    largest = bound if full else min(bound, max(-(-total // number_of), total * weights[0] // sum(weights)))
    least = 1 if total - largest >= number_of - 1 else 0
    holding, rest = [largest] + [least] * (number_of - 1), total - largest - least * (number_of - 1)
    while rest > 0:
        candidates = [i for i in range(1, number_of) if holding[i] < largest] or [i for i in range(1, number_of) if holding[i] < bound]
        whole, remaining = sum([weights[i] for i in candidates]), rest
        for i in candidates:
            addition = min(bound - holding[i], max(1, remaining * weights[i] // whole), rest)
            holding[i] = holding[i] + addition
            rest = rest - addition
    return np.array(holding)


def centred(key, dims, spread, limit, split=(), kind=jnp.bfloat16):
    drawn = jax.random.normal(key, dims, jnp.float32) * spread
    if len(split) > 0:
        drawn = level_of(key, dims, split, -0.22, 0.18) * drawn
    return jnp.clip(drawn, min=-limit, max=limit).astype(kind)


def setup_inputs(seed: int = 0) -> dict:
    streams_of = jax.random.split(jax.random.key(seed), 13)
    tokens = centred(streams_of[0], (TOKENS, D), 1.0, 6.0, ((0, 256),))
    cotangent = centred(streams_of[1], (TOKENS, D), 1.0, 6.0, ((0, 256),))
    gates = jnp.clip(jnp.exp(math.log(1.0) - 2.3025851 * jax.random.uniform(streams_of[2], (TOKENS, TOPK), jnp.float32) ** level_of(streams_of[2], (TOKENS, TOPK), ((0, 256),), -0.2, 0.2)), 0.1, 1.0)
    routes_keys = jax.random.split(jax.random.fold_in(streams_of[3], 1), TOKENS // TOK_DEV)
    routes_turns = jax.random.permutation(jax.random.fold_in(streams_of[3], 3), TOKENS // TOK_DEV)
    routes = jax.vmap(lambda own, number: deal_out(jax.random.fold_in(streams_of[3], 2), own, number, TOK_DEV, EXPERTS, TOPK, CAP, 1))(routes_keys, routes_turns).reshape((TOKENS, TOPK))
    w_up = centred(streams_of[4], (EXPERTS, D, FF), D ** -0.5, 0.09375, ((0, 32), (2, 8)))
    w_down = centred(streams_of[5], (EXPERTS, FF, D), FF ** -0.5, 0.1875, ((0, 32), (1, 8)))
    m_up = centred(streams_of[6], (EXPERTS, D, FF), 0.5, 3.0, ((0, 32), (2, 8)))
    v_up = jnp.clip(jnp.exp(math.log(1.0) - 2.306499 * jax.random.uniform(streams_of[7], (EXPERTS, D, FF), jnp.float32) ** level_of(streams_of[7], (EXPERTS, D, FF), ((0, 32), (2, 8)), -0.2, 0.2)), 0.099609375, 1.0).astype(jnp.bfloat16)
    m_down = centred(streams_of[8], (EXPERTS, FF, D), 0.5, 3.0, ((0, 32), (1, 8)))
    v_down = jnp.clip(jnp.exp(math.log(1.0) - 2.306499 * jax.random.uniform(streams_of[9], (EXPERTS, FF, D), jnp.float32) ** level_of(streams_of[9], (EXPERTS, FF, D), ((0, 32), (1, 8)), -0.2, 0.2)), 0.099609375, 1.0).astype(jnp.bfloat16)
    leaving = jax.random.randint(streams_of[10], (1,), 0, EXPERTS).astype(jnp.int32)
    tile_owner = jax.random.permutation(streams_of[11], EXPERTS).astype(jnp.int32)
    return {"tokens": tokens, "cotangent": cotangent, "gates": gates, "routes": routes, "w_up": w_up, "w_down": w_down, "m_up": m_up, "v_up": v_up, "m_down": m_down, "v_down": v_down, "leaving": leaving, "tile_owner": tile_owner}


BETA_ONE = 0.9
BETA_TWO = 0.95
EPSILON = 1e-08

def expert_terms(rows_x, rows_c, up_tile, down_tile):
    preact = jnp.dot(rows_x, up_tile, preferred_element_type=jnp.float32)
    squash = jax.nn.sigmoid(preact)
    hidden = (preact * squash).astype(jnp.bfloat16)
    slope_val = squash * (1.0 + preact * (1.0 - squash))
    back_grad = lax.dot_general(rows_c, down_tile, (((1,), (1,)), ((), ())), preferred_element_type=jnp.float32)
    pre_grad = (back_grad * slope_val).astype(jnp.bfloat16)
    grad_up = lax.dot_general(rows_x, pre_grad, (((0,), (0,)), ((), ())), preferred_element_type=jnp.float32)
    grad_cols = lax.dot_general(rows_c, hidden, (((0,), (0,)), ((), ())), preferred_element_type=jnp.float32)
    return (grad_up, grad_cols)

def adam_step(gradient, moment_one, moment_two):
    new_one = BETA_ONE * moment_one.astype(jnp.float32) + (1.0 - BETA_ONE) * gradient
    new_two = BETA_TWO * moment_two.astype(jnp.float32) + (1.0 - BETA_TWO) * gradient * gradient
    return (new_one / (jnp.sqrt(new_two) + EPSILON)).astype(jnp.bfloat16)

def reference(tokens, cotangent, gates, routes, w_up, w_down, m_up, v_up, m_down, v_down, leaving, tile_owner):
    experts = w_up.shape[0]
    hidden_units = w_up.shape[2]
    tok_count, model_width = tokens.shape
    top_count = routes.shape[1]
    pair_count = tok_count * top_count
    expert_of = routes.reshape(pair_count)
    pair_x = jnp.repeat(tokens, top_count, axis=0)
    pair_c = (gates.reshape(pair_count)[:, None] * jnp.repeat(cotangent, top_count, axis=0).astype(jnp.float32)).astype(jnp.bfloat16)
    most_rows = DEVICES * CAP

    def one_expert(expert_id):
        sort_key = jnp.where(expert_of == expert_id, 0, 1).astype(jnp.int32)
        row_order = jnp.argsort(sort_key, stable=True)[:most_rows]
        is_valid = (expert_of[row_order] == expert_id)[:, None]
        rows_x = jnp.where(is_valid, pair_x[row_order], jnp.zeros((), jnp.bfloat16))
        rows_c = jnp.where(is_valid, pair_c[row_order], jnp.zeros((), jnp.bfloat16))
        up_tile = lax.dynamic_index_in_dim(w_up, expert_id, 0, keepdims=False)
        down_tile = lax.dynamic_index_in_dim(w_down, expert_id, 0, keepdims=False)
        grad_up, grad_cols = expert_terms(rows_x, rows_c, up_tile, down_tile)
        step_up = adam_step(grad_up, lax.dynamic_index_in_dim(m_up, expert_id, 0, keepdims=False), lax.dynamic_index_in_dim(v_up, expert_id, 0, keepdims=False))
        step_down = adam_step(grad_cols.T, lax.dynamic_index_in_dim(m_down, expert_id, 0, keepdims=False), lax.dynamic_index_in_dim(v_down, expert_id, 0, keepdims=False))
        return (step_up, step_down)
    expert_ids = jnp.arange(experts, dtype=jnp.int32)
    steps_up, steps_down = lax.map(one_expert, expert_ids)
    leaver = leaving[0]
    keep_own = (expert_ids != leaver)[:, None, None]
    update_up = jnp.where(keep_own, steps_up, jnp.zeros((), jnp.bfloat16))
    update_down = jnp.where(keep_own, steps_down, jnp.zeros((), jnp.bfloat16))
    leaver_up = lax.dynamic_index_in_dim(steps_up, leaver, 0, keepdims=False)
    leaver_down = lax.dynamic_index_in_dim(steps_down, leaver, 0, keepdims=False)
    tile_rows = model_width // experts
    adopt = lax.optimization_barrier(jnp.sum(jnp.where(tile_owner[None, :] == expert_ids[:, None], expert_ids[None, :], 0), axis=1)).astype(jnp.int32)
    adopted_up = leaver_up.reshape(experts, tile_rows, hidden_units)[adopt]
    adopted_down = leaver_down.T.reshape(experts, tile_rows, hidden_units)[adopt]
    return (update_up, update_down, adopted_up, adopted_down)
```

```python
import functools

import jax
import jax.numpy as jnp
from jax import lax
from jax.experimental import pallas as pl
from jax.experimental.pallas import tpu as pltpu
from jax.sharding import PartitionSpec as P

BETA_ONE = 0.9
BETA_TWO = 0.95
EPSILON = 1e-08

MESH = pl.DeviceIdType.MESH
F32 = jnp.float32
BF16 = jnp.bfloat16

SLOTS = 5
COLS = 16
SIDE = 4
HALF = 4
RING = 8
PARTS = 4
WIDTH = 256
MSG = PARTS * 2 * SLOTS
UNIT = COLS * SLOTS
ALL = COLS * MSG


def mul_t(a, b):
    return lax.dot_general(a, b, (((1,), (1,)), ((), ())), preferred_element_type=F32)


def mul(a, b):
    return lax.dot_general(a, b, (((1,), (0,)), ((), ())), preferred_element_type=F32)


def adam_step(gradient, moment_one, moment_two):
    new_one = BETA_ONE * moment_one.astype(F32) + (1.0 - BETA_ONE) * gradient
    new_two = BETA_TWO * moment_two.astype(F32) + (1.0 - BETA_TWO) * gradient * gradient
    return new_one / (jnp.sqrt(new_two) + EPSILON)


def kernel(
    routes_ref, gates_ref, tok_hbm, cot_hbm, wup_hbm, wdn_hbm, mup_hbm, vup_hbm, mdn_hbm, vdn_hbm,
    sup_hbm, sdn_hbm,
    tok, cot, wup, wdn, mup, vup, mdn, vdn, sup, sdn,
    pick, unpick, packed, landed, own, other, transit, gup, gdn,
    load_sem, out_sem, plane_send, plane_recv, plane_self,
    chain_send, chain_recv, other_send, transit_send, transit_recv, mate_send, mate_recv,
):
    chunks = packed.shape[0]
    half_width = tok.shape[1] // 2
    dp = lax.axis_index("dp")
    ex = lax.axis_index("expert")
    core = lax.rem(dp, 2)
    pos = dp // 2
    zhi = lax.rem(ex, 2)
    col = ex // 2
    cy, cx = col // SIDE, lax.rem(col, SIDE)
    z = zhi * HALF + pos
    me_other = 1 - zhi

    def at_z(z_to):
        return ((z_to % HALF) * 2 + core, col * 2 + z_to // HALF)

    znext, zprev = lax.rem(z + 1, RING), lax.rem(z + RING - 1, RING)
    mate = (pos * 2 + (1 - core), ex)

    def peer_col(i):
        return lax.rem(cy + i // SIDE, SIDE) * SIDE + lax.rem(cx + i % SIDE, SIDE)

    barrier = pltpu.get_barrier_semaphore()
    for i in range(1, COLS):
        pl.semaphore_signal(
            barrier, inc=1, device_id=(dp, peer_col(i) * 2 + zhi), device_id_type=MESH
        )
    for who in (at_z(znext), at_z(zprev), mate):
        pl.semaphore_signal(barrier, inc=1, device_id=who, device_id_type=MESH)

    loads = [
        pltpu.make_async_copy(src, dst, load_sem.at[i])
        for i, (src, dst) in enumerate(
            (
                (tok_hbm, tok),
                (cot_hbm, cot),
                (wup_hbm, wup),
                (wdn_hbm, wdn),
                (mup_hbm, mup),
                (vup_hbm, vup),
                (mdn_hbm, mdn),
                (vdn_hbm, vdn),
            )
        )
    ]
    for load in loads:
        load.start()

    count = tok.shape[0]
    routes = routes_ref[...]
    expert_ids = lax.broadcasted_iota(jnp.int32, (2 * COLS, count), 0)
    member = (expert_ids == routes).astype(F32)
    before = (
        lax.broadcasted_iota(jnp.int32, (count, count), 0)
        < lax.broadcasted_iota(jnp.int32, (count, count), 1)
    ).astype(BF16)
    rank = jnp.sum(member * mul(member.astype(BF16), before), axis=0, keepdims=True)
    place = (routes >> 1) * MSG + (routes & 1) * SLOTS + rank.astype(jnp.int32)
    eye = lax.broadcasted_iota(jnp.int32, (count, count), 0) == lax.broadcasted_iota(
        jnp.int32, (count, count), 1
    )
    gates = jnp.sum(
        jnp.where(eye, jnp.broadcast_to(gates_ref[...], (count, count)), 0.0), axis=1, keepdims=True
    )
    target = lax.broadcasted_iota(jnp.int32, (ALL, count), 0)
    for part in range(PARTS):
        pick[:, part * count : (part + 1) * count] = (target == place + part * 2 * SLOTS).astype(
            F32
        ).astype(BF16)

    line = lax.broadcasted_iota(jnp.int32, (UNIT, ALL), 0)
    source = lax.broadcasted_iota(jnp.int32, (UNIT, ALL), 1)
    fifth = (line * 205) >> 10
    base = fifth * MSG + (line - fifth * SLOTS)
    for part in range(PARTS):
        for which, half in ((0, zhi), (1, me_other)):
            start = (part * 2 + which) * UNIT
            unpick[start : start + UNIT, :] = (
                (source == base + (part * 2 * SLOTS + half * SLOTS)).astype(F32).astype(BF16)
            )

    gup[...] = jnp.zeros_like(gup)
    gdn[...] = jnp.zeros_like(gdn)

    pl.semaphore_wait(barrier, COLS - 1 + 3)
    loads[0].wait()
    loads[1].wait()

    def lanes(chunk, high):
        return pl.ds(pl.multiple_of(high * half_width + chunk * WIDTH, 128), WIDTH)

    def plane_copy(chunk, i):
        to = peer_col(i)
        return pltpu.make_async_remote_copy(
            src_ref=packed.at[chunk, to],
            dst_ref=landed.at[chunk, col],
            send_sem=plane_send.at[chunk, i],
            recv_sem=plane_recv.at[chunk, i],
            device_id=(dp, to * 2 + zhi),
            device_id_type=MESH,
        )

    def plane_keep(chunk):
        return pltpu.make_async_copy(
            packed.at[chunk, col], landed.at[chunk, col], plane_self.at[chunk]
        )

    @pl.loop(0, chunks)
    def _(chunk):
        both = [tok[:, lanes(chunk, h)] for h in range(2)]
        both += [
            (gates * cot[:, lanes(chunk, h)].astype(F32)).astype(BF16) for h in range(2)
        ]
        rows = mul(pick[...], jnp.concatenate(both, axis=0))
        packed[chunk] = rows.reshape(COLS, MSG, WIDTH).astype(BF16)
        plane_keep(chunk).start()

        @pl.loop(1, COLS)
        def _(i):
            plane_copy(chunk, i).start()

    def chain(slot, chunk, to_next, own_side):
        z_to = jnp.where(to_next, znext, zprev)
        return pltpu.make_async_remote_copy(
            src_ref=own.at[slot, core, chunk],
            dst_ref=own.at[slot, core, chunk],
            send_sem=chain_send.at[own_side, slot, chunk],
            recv_sem=chain_recv.at[slot, chunk],
            device_id=at_z(z_to),
            device_id_type=MESH,
        )

    def hand_over(slot, chunk):
        return pltpu.make_async_remote_copy(
            src_ref=own.at[slot, core, chunk],
            dst_ref=own.at[slot, core, chunk],
            send_sem=mate_send.at[slot, chunk],
            recv_sem=mate_recv.at[slot, chunk],
            device_id=mate,
            device_id_type=MESH,
        )

    upper = pos >= 2
    edge = (pos == 0) | (pos == HALF - 1)
    z_out = jnp.where(upper, znext, zprev)

    def other_inner(chunk):
        return pltpu.make_async_remote_copy(
            src_ref=other.at[chunk],
            dst_ref=transit.at[chunk],
            send_sem=other_send.at[chunk],
            recv_sem=transit_recv.at[chunk],
            device_id=at_z(z_out),
            device_id_type=MESH,
        )

    def other_edge(chunk):
        return pltpu.make_async_remote_copy(
            src_ref=other.at[chunk],
            dst_ref=own.at[z, core, chunk],
            send_sem=other_send.at[chunk],
            recv_sem=chain_recv.at[z, chunk],
            device_id=at_z(z_out),
            device_id_type=MESH,
        )

    z_via = jnp.where(upper, zprev, znext)

    def transit_edge(chunk):
        return pltpu.make_async_remote_copy(
            src_ref=transit.at[chunk],
            dst_ref=own.at[z_via, core, chunk],
            send_sem=transit_send.at[chunk],
            recv_sem=chain_recv.at[z_via, chunk],
            device_id=at_z(z_out),
            device_id_type=MESH,
        )

    @pl.loop(0, chunks)
    def _(chunk):
        plane_keep(chunk).wait()

        @pl.loop(1, COLS)
        def _(i):
            plane_copy(chunk, i).wait_recv()

        rows = mul(
            unpick[...], landed[chunk].astype(F32).reshape(ALL, WIDTH).astype(BF16)
        ).astype(BF16)
        for part in range(PARTS):
            start = part * 2 * UNIT
            own[z, core, chunk, :, part * WIDTH : (part + 1) * WIDTH] = rows[start : start + UNIT]
            other[chunk, :, part * WIDTH : (part + 1) * WIDTH] = rows[
                start + UNIT : start + 2 * UNIT
            ]

        @pl.when(edge)
        def _():
            other_edge(chunk).start()

        @pl.when(jnp.logical_not(edge))
        def _():
            other_inner(chunk).start()

        @pl.when(pos < HALF - 1)
        def _():
            chain(z, chunk, True, 1).start()

        @pl.when(pos > 0)
        def _():
            chain(z, chunk, False, 0).start()

        hand_over(z, chunk).start()

    for load in loads[2:]:
        load.wait()

    def pair(slot, chunk):
        return jnp.concatenate([own[slot, 0, chunk], own[slot, 1, chunk]], axis=0)

    def terms(slot):
        preact = jnp.zeros((2 * UNIT, wup.shape[1]), F32)
        back = jnp.zeros((2 * UNIT, wup.shape[1]), F32)
        for chunk in range(chunks):
            rows = pair(slot, chunk)
            for high in range(2):
                at = high * half_width + chunk * WIDTH
                preact += mul(
                    rows[:, high * WIDTH : (high + 1) * WIDTH], wup[at : at + WIDTH, :]
                )
                back += mul_t(
                    rows[:, (2 + high) * WIDTH : (3 + high) * WIDTH], wdn[:, at : at + WIDTH]
                )
        squash = jax.nn.sigmoid(preact)
        hidden = preact * squash
        pre_grad = back * (squash * (1.0 + preact * (1.0 - squash)))
        hidden = hidden.astype(BF16).astype(F32).T.astype(BF16)
        pre_grad = pre_grad.astype(BF16).astype(F32).T.astype(BF16)
        for chunk in range(chunks):
            rows = pair(slot, chunk)
            for high in range(2):
                at = high * half_width + chunk * WIDTH
                gup[:, at : at + WIDTH] += mul(
                    pre_grad, rows[:, high * WIDTH : (high + 1) * WIDTH]
                )
                gdn[:, at : at + WIDTH] += mul(
                    hidden, rows[:, (2 + high) * WIDTH : (3 + high) * WIDTH]
                )

    def finish(slot):
        @pl.loop(0, chunks)
        def _(chunk):
            hand_over(slot, chunk).wait_recv()

        terms(slot)

    @pl.when(edge)
    def _():
        @pl.loop(0, chunks)
        def _(chunk):
            other_inner(chunk).wait_recv()
            transit_edge(chunk).start()

    finish(z)

    @pl.loop(0, 10)
    def _(j):
        far = j // 2 + 1
        from_prev = (lax.rem(j, 2) == 1) == upper
        reach = jnp.where(from_prev, pos + 2, HALF + 1 - pos)

        @pl.when(far <= reach)
        def _():
            slot = lax.rem(jnp.where(from_prev, z + RING - far, z + far), RING)
            onward = jnp.where(from_prev, pos < HALF - 1, pos > 0)

            @pl.loop(0, chunks)
            def _(chunk):
                chain(slot, chunk, from_prev, 0).wait_recv()

                @pl.when(onward)
                def _():
                    chain(slot, chunk, from_prev, 0).start()

                hand_over(slot, chunk).start()

            finish(slot)

    model_width = tok.shape[1]
    block = 128

    @pl.loop(0, model_width // block)
    def _(b):
        at = pl.ds(pl.multiple_of(b * block, block), block)
        sup[at, :] = adam_step(gup[:, at].T, mup[at, :], vup[at, :]).astype(BF16)
        sdn[:, at] = adam_step(gdn[:, at], mdn[:, at], vdn[:, at]).astype(BF16)

    outs = [
        pltpu.make_async_copy(sup, sup_hbm, out_sem.at[0]),
        pltpu.make_async_copy(sdn, sdn_hbm, out_sem.at[1]),
    ]
    for out in outs:
        out.start()

    @pl.loop(0, chunks)
    def _(chunk):
        @pl.loop(1, COLS)
        def _(i):
            plane_copy(chunk, i).wait_send()

        other_inner(chunk).wait_send()
        hand_over(z, chunk).wait_send()

        @pl.when(edge)
        def _():
            transit_edge(chunk).wait_send()

        @pl.when(pos < HALF - 1)
        def _():
            chain(z, chunk, True, 1).wait_send()

        @pl.when(pos > 0)
        def _():
            chain(z, chunk, False, 0).wait_send()

    @pl.loop(0, 10)
    def _(j):
        far = j // 2 + 1
        from_prev = (lax.rem(j, 2) == 1) == upper
        reach = jnp.where(from_prev, pos + 2, HALF + 1 - pos)

        @pl.when(far <= reach)
        def _():
            slot = lax.rem(jnp.where(from_prev, z + RING - far, z + far), RING)
            onward = jnp.where(from_prev, pos < HALF - 1, pos > 0)

            @pl.loop(0, chunks)
            def _(chunk):
                @pl.when(onward)
                def _():
                    chain(slot, chunk, from_prev, 0).wait_send()

                hand_over(slot, chunk).wait_send()

    for out in outs:
        out.wait()


def expert_steps(routes, gates, tokens, cotangent, w_up, w_down, m_up, v_up, m_down, v_down):
    count, model_width = tokens.shape
    hidden = w_up.shape[1]
    chunks = model_width // 2 // WIDTH
    vmem = pl.BlockSpec(memory_space=pltpu.VMEM)
    anyw = pl.BlockSpec(memory_space=pl.ANY)
    dma = pltpu.SemaphoreType.DMA
    return pl.pallas_call(
        kernel,
        out_shape=(
            jax.ShapeDtypeStruct((model_width, hidden), BF16),
            jax.ShapeDtypeStruct((hidden, model_width), BF16),
        ),
        in_specs=[vmem, vmem] + [anyw] * 8,
        out_specs=(anyw, anyw),
        scratch_shapes=[
            pltpu.VMEM((count, model_width), BF16),
            pltpu.VMEM((count, model_width), BF16),
            pltpu.VMEM((model_width, hidden), BF16),
            pltpu.VMEM((hidden, model_width), BF16),
            pltpu.VMEM((model_width, hidden), BF16),
            pltpu.VMEM((model_width, hidden), BF16),
            pltpu.VMEM((hidden, model_width), BF16),
            pltpu.VMEM((hidden, model_width), BF16),
            pltpu.VMEM((model_width, hidden), BF16),
            pltpu.VMEM((hidden, model_width), BF16),
            pltpu.VMEM((ALL, PARTS * count), BF16),
            pltpu.VMEM((PARTS * 2 * UNIT, ALL), BF16),
            pltpu.VMEM((chunks, COLS, MSG, WIDTH), BF16),
            pltpu.VMEM((chunks, COLS, MSG, WIDTH), BF16),
            pltpu.VMEM((RING, 2, chunks, UNIT, PARTS * WIDTH), BF16),
            pltpu.VMEM((chunks, UNIT, PARTS * WIDTH), BF16),
            pltpu.VMEM((chunks, UNIT, PARTS * WIDTH), BF16),
            pltpu.VMEM((hidden, model_width), F32),
            pltpu.VMEM((hidden, model_width), F32),
            dma((8,)),
            dma((2,)),
            dma((chunks, COLS)),
            dma((chunks, COLS)),
            dma((chunks,)),
            dma((2, RING, chunks)),
            dma((RING, chunks)),
            dma((chunks,)),
            dma((chunks,)),
            dma((chunks,)),
            dma((RING, chunks)),
            dma((RING, chunks)),
        ],
        compiler_params=pltpu.CompilerParams(
            collective_id=0, has_side_effects=True, vmem_limit_bytes=60 * 1024 * 1024
        ),
        name="expert_steps",
    )(routes, gates, tokens, cotangent, w_up, w_down, m_up, v_up, m_down, v_down)


def on_device(
    tokens, cotangent, gates, routes, w_up, w_down, m_up, v_up, m_down, v_down, leaving, tile_owner
):
    experts = lax.axis_size("expert")
    my_index = lax.axis_index("expert")
    tok_count, model_width = tokens.shape
    hidden_units = w_up.shape[2]
    leaver = leaving[0]
    slot_ids = jnp.arange(experts, dtype=jnp.int32)
    tile_rows = model_width // experts
    adopt = jnp.sum(
        jnp.where(tile_owner[None, :] == slot_ids[:, None], slot_ids[None, :], 0), axis=1
    )
    step_up, step_down = expert_steps(
        routes.reshape(1, tok_count),
        gates.reshape(1, tok_count),
        tokens,
        cotangent,
        w_up[0],
        w_down[0],
        m_up[0],
        v_up[0],
        m_down[0],
        v_down[0],
    )
    keep_own = my_index != leaver
    both_steps = jnp.concatenate([step_up, step_down.T], axis=1).reshape(
        experts, tile_rows, 2 * hidden_units
    )
    ordered = both_steps[adopt]
    outgoing = jnp.where(keep_own, jnp.zeros_like(ordered), ordered)
    incoming = lax.all_to_all(outgoing, "expert", split_axis=0, concat_axis=0, tiled=True)
    mine = lax.dynamic_index_in_dim(incoming, leaver, 0, keepdims=False)
    adopted_up = mine[:, :hidden_units][None]
    adopted_down = mine[:, hidden_units:][None]
    update_up = jnp.where(keep_own, step_up, jnp.zeros_like(step_up))[None]
    update_down = jnp.where(keep_own, step_down, jnp.zeros_like(step_down))[None]
    return (update_up, update_down, adopted_up, adopted_down)


def solution(mesh):
    placed = (
        P(("dp", "expert"), None),
        P(("dp", "expert"), None),
        P(("dp", "expert"), None),
        P(("dp", "expert"), None),
        P("expert", None, "dp"),
        P("expert", "dp", None),
        P("expert", None, "dp"),
        P("expert", None, "dp"),
        P("expert", "dp", None),
        P("expert", "dp", None),
        P(),
        P(),
    )
    return jax.shard_map(
        on_device,
        mesh=mesh,
        in_specs=placed,
        out_specs=(
            P("expert", None, "dp"),
            P("expert", "dp", None),
            P("expert", None, "dp"),
            P("expert", None, "dp"),
        ),
        check_vma=False,
    )
```

```python
import functools

import jax
import jax.numpy as jnp
from jax import lax
from jax.experimental import pallas as pl
from jax.experimental.pallas import tpu as pltpu
from jax.sharding import PartitionSpec as P

BETA_ONE = 0.9
BETA_TWO = 0.95
EPSILON = 1e-08

MESH = pl.DeviceIdType.MESH
F32 = jnp.float32
BF16 = jnp.bfloat16

SLOTS = 5
COLS = 16
SIDE = 4
HALF = 4
RING = 8
PARTS = 4
WIDTH = 256
MSG = PARTS * 2 * SLOTS
UNIT = COLS * SLOTS
ALL = COLS * MSG


def mul_t(a, b):
    return lax.dot_general(a, b, (((1,), (1,)), ((), ())), preferred_element_type=F32)


def mul(a, b):
    return lax.dot_general(a, b, (((1,), (0,)), ((), ())), preferred_element_type=F32)


def adam_step(gradient, moment_one, moment_two):
    new_one = BETA_ONE * moment_one.astype(F32) + (1.0 - BETA_ONE) * gradient
    new_two = BETA_TWO * moment_two.astype(F32) + (1.0 - BETA_TWO) * gradient * gradient
    return new_one / (jnp.sqrt(new_two) + EPSILON)


def kernel(
    leaving_ref, adopt_ref, routes_ref, gates_ref, tok_hbm, cot_hbm, wup_hbm, wdn_hbm, mup_hbm, vup_hbm, mdn_hbm, vdn_hbm,
    sup_hbm, sdn_hbm, aup_ref, adn_ref,
    tok, cot, wup, wdn, mup, vup, mdn, vdn, sup, sdn,
    pick, unpick, packed, landed, own, other, transit, gup, gdn,
    leave_up, leave_dn, by_tile, tiles, hop, got, summed, fin, last,
    load_sem, out_sem, plane_send, plane_recv, plane_self,
    chain_send, chain_recv, other_send, transit_send, transit_recv, mate_send, mate_recv,
    hop_send, hop_recv, ring_send, ring_recv, fin_send, fin_recv, last_send, last_recv,
):
    chunks = packed.shape[0]
    half_width = tok.shape[1] // 2
    dp = lax.axis_index("dp")
    ex = lax.axis_index("expert")
    core = lax.rem(dp, 2)
    pos = dp // 2
    zhi = lax.rem(ex, 2)
    col = ex // 2
    cy, cx = col // SIDE, lax.rem(col, SIDE)
    z = zhi * HALF + pos
    me_other = 1 - zhi

    def at_z(z_to):
        return ((z_to % HALF) * 2 + core, col * 2 + z_to // HALF)

    znext, zprev = lax.rem(z + 1, RING), lax.rem(z + RING - 1, RING)
    mate = (pos * 2 + (1 - core), ex)

    def peer_col(i):
        return lax.rem(cy + i // SIDE, SIDE) * SIDE + lax.rem(cx + i % SIDE, SIDE)

    barrier = pltpu.get_barrier_semaphore()
    for i in range(1, COLS):
        pl.semaphore_signal(
            barrier, inc=1, device_id=(dp, peer_col(i) * 2 + zhi), device_id_type=MESH
        )
    twin = (dp, col * 2 + me_other)
    for who in (at_z(znext), at_z(zprev), mate, twin):
        pl.semaphore_signal(barrier, inc=1, device_id=who, device_id_type=MESH)

    loads = [
        pltpu.make_async_copy(src, dst, load_sem.at[i])
        for i, (src, dst) in enumerate(
            (
                (tok_hbm, tok),
                (cot_hbm, cot),
                (wup_hbm, wup),
                (wdn_hbm, wdn),
                (mup_hbm, mup),
                (vup_hbm, vup),
                (mdn_hbm, mdn),
                (vdn_hbm, vdn),
            )
        )
    ]
    for load in loads:
        load.start()

    count = tok.shape[0]
    routes = routes_ref[...]
    expert_ids = lax.broadcasted_iota(jnp.int32, (2 * COLS, count), 0)
    member = (expert_ids == routes).astype(F32)
    before = (
        lax.broadcasted_iota(jnp.int32, (count, count), 0)
        < lax.broadcasted_iota(jnp.int32, (count, count), 1)
    ).astype(BF16)
    rank = jnp.sum(member * mul(member.astype(BF16), before), axis=0, keepdims=True)
    place = (routes >> 1) * MSG + (routes & 1) * SLOTS + rank.astype(jnp.int32)
    eye = lax.broadcasted_iota(jnp.int32, (count, count), 0) == lax.broadcasted_iota(
        jnp.int32, (count, count), 1
    )
    gates = jnp.sum(
        jnp.where(eye, jnp.broadcast_to(gates_ref[...], (count, count)), 0.0), axis=1, keepdims=True
    )
    target = lax.broadcasted_iota(jnp.int32, (ALL, count), 0)
    for part in range(PARTS):
        pick[:, part * count : (part + 1) * count] = (target == place + part * 2 * SLOTS).astype(
            F32
        ).astype(BF16)

    line = lax.broadcasted_iota(jnp.int32, (UNIT, ALL), 0)
    source = lax.broadcasted_iota(jnp.int32, (UNIT, ALL), 1)
    fifth = (line * 205) >> 10
    base = fifth * MSG + (line - fifth * SLOTS)
    for part in range(PARTS):
        for which, half in ((0, zhi), (1, me_other)):
            start = (part * 2 + which) * UNIT
            unpick[start : start + UNIT, :] = (
                (source == base + (part * 2 * SLOTS + half * SLOTS)).astype(F32).astype(BF16)
            )

    gup[...] = jnp.zeros_like(gup)
    gdn[...] = jnp.zeros_like(gdn)

    pl.semaphore_wait(barrier, COLS - 1 + 4)
    loads[0].wait()
    loads[1].wait()

    def lanes(chunk, high):
        return pl.ds(pl.multiple_of(high * half_width + chunk * WIDTH, 128), WIDTH)

    def plane_copy(chunk, i):
        to = peer_col(i)
        return pltpu.make_async_remote_copy(
            src_ref=packed.at[chunk, to],
            dst_ref=landed.at[chunk, col],
            send_sem=plane_send.at[chunk, i],
            recv_sem=plane_recv.at[chunk, i],
            device_id=(dp, to * 2 + zhi),
            device_id_type=MESH,
        )

    def plane_keep(chunk):
        return pltpu.make_async_copy(
            packed.at[chunk, col], landed.at[chunk, col], plane_self.at[chunk]
        )

    @pl.loop(0, chunks)
    def _(chunk):
        both = [tok[:, lanes(chunk, h)] for h in range(2)]
        both += [
            (gates * cot[:, lanes(chunk, h)].astype(F32)).astype(BF16) for h in range(2)
        ]
        rows = mul(pick[...], jnp.concatenate(both, axis=0))
        packed[chunk] = rows.reshape(COLS, MSG, WIDTH).astype(BF16)
        plane_keep(chunk).start()

        @pl.loop(1, COLS)
        def _(i):
            plane_copy(chunk, i).start()

    def chain(slot, chunk, to_next, own_side):
        z_to = jnp.where(to_next, znext, zprev)
        return pltpu.make_async_remote_copy(
            src_ref=own.at[slot, core, chunk],
            dst_ref=own.at[slot, core, chunk],
            send_sem=chain_send.at[own_side, slot, chunk],
            recv_sem=chain_recv.at[slot, chunk],
            device_id=at_z(z_to),
            device_id_type=MESH,
        )

    def hand_over(slot, chunk):
        return pltpu.make_async_remote_copy(
            src_ref=own.at[slot, core, chunk],
            dst_ref=own.at[slot, core, chunk],
            send_sem=mate_send.at[slot, chunk],
            recv_sem=mate_recv.at[slot, chunk],
            device_id=mate,
            device_id_type=MESH,
        )

    upper = pos >= 2
    edge = (pos == 0) | (pos == HALF - 1)
    z_out = jnp.where(upper, znext, zprev)

    def other_inner(chunk):
        return pltpu.make_async_remote_copy(
            src_ref=other.at[chunk],
            dst_ref=transit.at[chunk],
            send_sem=other_send.at[chunk],
            recv_sem=transit_recv.at[chunk],
            device_id=at_z(z_out),
            device_id_type=MESH,
        )

    def other_edge(chunk):
        return pltpu.make_async_remote_copy(
            src_ref=other.at[chunk],
            dst_ref=own.at[z, core, chunk],
            send_sem=other_send.at[chunk],
            recv_sem=chain_recv.at[z, chunk],
            device_id=at_z(z_out),
            device_id_type=MESH,
        )

    z_via = jnp.where(upper, zprev, znext)

    def transit_edge(chunk):
        return pltpu.make_async_remote_copy(
            src_ref=transit.at[chunk],
            dst_ref=own.at[z_via, core, chunk],
            send_sem=transit_send.at[chunk],
            recv_sem=chain_recv.at[z_via, chunk],
            device_id=at_z(z_out),
            device_id_type=MESH,
        )

    @pl.loop(0, chunks)
    def _(chunk):
        plane_keep(chunk).wait()

        @pl.loop(1, COLS)
        def _(i):
            plane_copy(chunk, i).wait_recv()

        rows = mul(
            unpick[...], landed[chunk].astype(F32).reshape(ALL, WIDTH).astype(BF16)
        ).astype(BF16)
        for part in range(PARTS):
            start = part * 2 * UNIT
            own[z, core, chunk, :, part * WIDTH : (part + 1) * WIDTH] = rows[start : start + UNIT]
            other[chunk, :, part * WIDTH : (part + 1) * WIDTH] = rows[
                start + UNIT : start + 2 * UNIT
            ]

        @pl.when(edge)
        def _():
            other_edge(chunk).start()

        @pl.when(jnp.logical_not(edge))
        def _():
            other_inner(chunk).start()

        @pl.when(pos < HALF - 1)
        def _():
            chain(z, chunk, True, 1).start()

        @pl.when(pos > 0)
        def _():
            chain(z, chunk, False, 0).start()

        hand_over(z, chunk).start()

    for load in loads[2:]:
        load.wait()

    def pair(slot, chunk):
        return jnp.concatenate([own[slot, 0, chunk], own[slot, 1, chunk]], axis=0)

    def terms(slot):
        preact = jnp.zeros((2 * UNIT, wup.shape[1]), F32)
        back = jnp.zeros((2 * UNIT, wup.shape[1]), F32)
        for chunk in range(chunks):
            rows = pair(slot, chunk)
            for high in range(2):
                at = high * half_width + chunk * WIDTH
                preact += mul(
                    rows[:, high * WIDTH : (high + 1) * WIDTH], wup[at : at + WIDTH, :]
                )
                back += mul_t(
                    rows[:, (2 + high) * WIDTH : (3 + high) * WIDTH], wdn[:, at : at + WIDTH]
                )
        squash = jax.nn.sigmoid(preact)
        hidden = preact * squash
        pre_grad = back * (squash * (1.0 + preact * (1.0 - squash)))
        hidden = hidden.astype(BF16).astype(F32).T.astype(BF16)
        pre_grad = pre_grad.astype(BF16).astype(F32).T.astype(BF16)
        for chunk in range(chunks):
            rows = pair(slot, chunk)
            for high in range(2):
                at = high * half_width + chunk * WIDTH
                gup[:, at : at + WIDTH] += mul(
                    pre_grad, rows[:, high * WIDTH : (high + 1) * WIDTH]
                )
                gdn[:, at : at + WIDTH] += mul(
                    hidden, rows[:, (2 + high) * WIDTH : (3 + high) * WIDTH]
                )

    def finish(slot):
        @pl.loop(0, chunks)
        def _(chunk):
            hand_over(slot, chunk).wait_recv()

        terms(slot)

    @pl.when(edge)
    def _():
        @pl.loop(0, chunks)
        def _(chunk):
            other_inner(chunk).wait_recv()
            transit_edge(chunk).start()

    finish(z)

    @pl.loop(0, 10)
    def _(j):
        far = j // 2 + 1
        from_prev = (lax.rem(j, 2) == 1) == upper
        reach = jnp.where(from_prev, pos + 2, HALF + 1 - pos)

        @pl.when(far <= reach)
        def _():
            slot = lax.rem(jnp.where(from_prev, z + RING - far, z + far), RING)
            onward = jnp.where(from_prev, pos < HALF - 1, pos > 0)

            @pl.loop(0, chunks)
            def _(chunk):
                chain(slot, chunk, from_prev, 0).wait_recv()

                @pl.when(onward)
                def _():
                    chain(slot, chunk, from_prev, 0).start()

                hand_over(slot, chunk).start()

            finish(slot)

    model_width = tok.shape[1]
    block = 128
    leaves = jnp.broadcast_to(leaving_ref[...], (block, block)) == ex
    ring_at, line_at = (cx, cy), (cy, cx)
    middle = SIDE

    def tile_home(axis, ring_to, line_to):
        to = line_to * SIDE + ring_to if axis == 0 else ring_to * SIDE + line_to
        return (dp, to * 2 + zhi)

    def ring_next(axis, far):
        return lax.rem(ring_at[axis] + far, SIDE)

    def ring_to(axis, side):
        return tile_home(axis, ring_next(axis, 1 if side == 0 else SIDE - 1), line_at[axis])

    def part_of(side):
        return pl.ds(0, middle) if side == 0 else pl.ds(middle, middle)

    def hop_copy(axis, side):
        return pltpu.make_async_remote_copy(
            src_ref=tiles.at[axis, ring_next(axis, 2), part_of(side)],
            dst_ref=hop.at[axis, side],
            send_sem=hop_send.at[axis, side],
            recv_sem=hop_recv.at[axis, side],
            device_id=ring_to(axis, side),
            device_id_type=MESH,
        )

    def ring_copy(axis, side, late):
        part = part_of(side if late else 1 - side)
        return pltpu.make_async_remote_copy(
            src_ref=tiles.at[axis, ring_next(axis, 1 if side == 0 else SIDE - 1), part],
            dst_ref=got.at[axis, side, part],
            send_sem=ring_send.at[axis, side, late],
            recv_sem=ring_recv.at[axis, side, late],
            device_id=ring_to(axis, side),
            device_id_type=MESH,
        )

    def fin_copy(axis, far):
        line_to = lax.rem(line_at[axis] + far, SIDE)
        return pltpu.make_async_remote_copy(
            src_ref=summed.at[axis, pl.ds(line_to * 2, 2)],
            dst_ref=fin.at[axis, far - 1],
            send_sem=fin_send.at[axis, far - 1],
            recv_sem=fin_recv.at[axis, far - 1],
            device_id=tile_home(axis, ring_at[axis], line_to),
            device_id_type=MESH,
        )

    def last_copy(axis):
        return pltpu.make_async_remote_copy(
            src_ref=summed.at[axis, line_at[axis] * 2 + me_other],
            dst_ref=last.at[axis],
            send_sem=last_send.at[axis],
            recv_sem=last_recv.at[axis],
            device_id=twin,
            device_id_type=MESH,
        )

    def sort_tiles(axis, leave):
        rows = tiles.shape[3]
        for tile in range(2 * COLS):
            by_tile[tile] = leave[tile * rows : (tile + 1) * rows, :]

        @pl.loop(0, 2 * COLS)
        def _(owner):
            to = owner // 2
            ty, tx = to // SIDE, lax.rem(to, SIDE)
            r, l = (tx, ty) if axis == 0 else (ty, tx)
            tiles[axis, r, l * 2 + lax.rem(owner, 2)] = by_tile[adopt_ref[owner]]

        for side in range(2):
            hop_copy(axis, side).start()
        for side in range(2):
            ring_copy(axis, side, 0).start()

    @pl.loop(0, model_width // block)
    def _(b):
        at = pl.ds(pl.multiple_of(b * block, block), block)
        step = adam_step(gup[:, at].T, mup[at, :], vup[at, :])
        sup[at, :] = jnp.where(leaves, 0.0, step).astype(BF16)
        leave_up[at, :] = jnp.where(leaves, step, 0.0).astype(BF16)

    out_up = pltpu.make_async_copy(sup, sup_hbm, out_sem.at[0])
    out_up.start()
    sort_tiles(0, leave_up)

    @pl.loop(0, model_width // block)
    def _(b):
        at = pl.ds(pl.multiple_of(b * block, block), block)
        step = adam_step(gdn[:, at], mdn[:, at], vdn[:, at])
        sdn[:, at] = jnp.where(leaves, 0.0, step).astype(BF16)
        leave_dn[at, :] = jnp.where(leaves, step, 0.0).T.astype(BF16)

    out_dn = pltpu.make_async_copy(sdn, sdn_hbm, out_sem.at[1])
    out_dn.start()
    sort_tiles(1, leave_dn)

    for axis in range(2):
        for side in range(2):
            hop_copy(axis, side).wait_recv()
            to = ring_next(axis, 1 if side == 0 else SIDE - 1)
            part = part_of(side)
            tiles[axis, to, part] = tiles[axis, to, part] + hop[axis, side]
            ring_copy(axis, side, 1).start()

    for axis in range(2):
        for side in range(2):
            for late in range(2):
                ring_copy(axis, side, late).wait_recv()
        summed[axis] = tiles[axis, ring_at[axis]] + got[axis, 0] + got[axis, 1]
        for far in range(1, SIDE):
            fin_copy(axis, far).start()

    for axis in range(2):
        for far in range(1, SIDE):
            fin_copy(axis, far).wait_recv()
        mine = pl.ds(line_at[axis] * 2, 2)
        summed[axis, mine] = summed[axis, mine] + fin[axis, 0] + fin[axis, 1] + fin[axis, 2]
        last_copy(axis).start()

    for axis, adopted in ((0, aup_ref), (1, adn_ref)):
        last_copy(axis).wait_recv()
        adopted[...] = summed[axis, line_at[axis] * 2 + zhi] + last[axis]

    for axis in range(2):
        for side in range(2):
            hop_copy(axis, side).wait_send()
            for late in range(2):
                ring_copy(axis, side, late).wait_send()
        for far in range(1, SIDE):
            fin_copy(axis, far).wait_send()
        last_copy(axis).wait_send()

    @pl.loop(0, chunks)
    def _(chunk):
        @pl.loop(1, COLS)
        def _(i):
            plane_copy(chunk, i).wait_send()

        other_inner(chunk).wait_send()
        hand_over(z, chunk).wait_send()

        @pl.when(edge)
        def _():
            transit_edge(chunk).wait_send()

        @pl.when(pos < HALF - 1)
        def _():
            chain(z, chunk, True, 1).wait_send()

        @pl.when(pos > 0)
        def _():
            chain(z, chunk, False, 0).wait_send()

    @pl.loop(0, 10)
    def _(j):
        far = j // 2 + 1
        from_prev = (lax.rem(j, 2) == 1) == upper
        reach = jnp.where(from_prev, pos + 2, HALF + 1 - pos)

        @pl.when(far <= reach)
        def _():
            slot = lax.rem(jnp.where(from_prev, z + RING - far, z + far), RING)
            onward = jnp.where(from_prev, pos < HALF - 1, pos > 0)

            @pl.loop(0, chunks)
            def _(chunk):
                @pl.when(onward)
                def _():
                    chain(slot, chunk, from_prev, 0).wait_send()

                hand_over(slot, chunk).wait_send()

    out_up.wait()
    out_dn.wait()


def expert_steps(leaving, adopt, routes, gates, tokens, cotangent, w_up, w_down, m_up, v_up, m_down, v_down):
    count, model_width = tokens.shape
    hidden = w_up.shape[1]
    chunks = model_width // 2 // WIDTH
    tile_rows = model_width // adopt.shape[0]
    smem = pl.BlockSpec(memory_space=pltpu.SMEM)
    vmem = pl.BlockSpec(memory_space=pltpu.VMEM)
    anyw = pl.BlockSpec(memory_space=pl.ANY)
    dma = pltpu.SemaphoreType.DMA
    return pl.pallas_call(
        kernel,
        out_shape=(
            jax.ShapeDtypeStruct((model_width, hidden), BF16),
            jax.ShapeDtypeStruct((hidden, model_width), BF16),
            jax.ShapeDtypeStruct((tile_rows, hidden), BF16),
            jax.ShapeDtypeStruct((tile_rows, hidden), BF16),
        ),
        in_specs=[vmem, smem, vmem, vmem] + [anyw] * 8,
        out_specs=(anyw, anyw, vmem, vmem),
        scratch_shapes=[
            pltpu.VMEM((count, model_width), BF16),
            pltpu.VMEM((count, model_width), BF16),
            pltpu.VMEM((model_width, hidden), BF16),
            pltpu.VMEM((hidden, model_width), BF16),
            pltpu.VMEM((model_width, hidden), BF16),
            pltpu.VMEM((model_width, hidden), BF16),
            pltpu.VMEM((hidden, model_width), BF16),
            pltpu.VMEM((hidden, model_width), BF16),
            pltpu.VMEM((model_width, hidden), BF16),
            pltpu.VMEM((hidden, model_width), BF16),
            pltpu.VMEM((ALL, PARTS * count), BF16),
            pltpu.VMEM((PARTS * 2 * UNIT, ALL), BF16),
            pltpu.VMEM((chunks, COLS, MSG, WIDTH), BF16),
            pltpu.VMEM((chunks, COLS, MSG, WIDTH), BF16),
            pltpu.VMEM((RING, 2, chunks, UNIT, PARTS * WIDTH), BF16),
            pltpu.VMEM((chunks, UNIT, PARTS * WIDTH), BF16),
            pltpu.VMEM((chunks, UNIT, PARTS * WIDTH), BF16),
            pltpu.VMEM((hidden, model_width), F32),
            pltpu.VMEM((hidden, model_width), F32),
            pltpu.VMEM((model_width, hidden), BF16),
            pltpu.VMEM((model_width, hidden), BF16),
            pltpu.VMEM((2 * COLS, tile_rows, hidden), BF16),
            pltpu.VMEM((2, SIDE, 2 * SIDE, tile_rows, hidden), BF16),
            pltpu.VMEM((2, 2, SIDE, tile_rows, hidden), BF16),
            pltpu.VMEM((2, 2, 2 * SIDE, tile_rows, hidden), BF16),
            pltpu.VMEM((2, 2 * SIDE, tile_rows, hidden), BF16),
            pltpu.VMEM((2, SIDE - 1, 2, tile_rows, hidden), BF16),
            pltpu.VMEM((2, tile_rows, hidden), BF16),
            dma((8,)),
            dma((2,)),
            dma((chunks, COLS)),
            dma((chunks, COLS)),
            dma((chunks,)),
            dma((2, RING, chunks)),
            dma((RING, chunks)),
            dma((chunks,)),
            dma((chunks,)),
            dma((chunks,)),
            dma((RING, chunks)),
            dma((RING, chunks)),
            dma((2, 2)),
            dma((2, 2)),
            dma((2, 2, 2)),
            dma((2, 2, 2)),
            dma((2, SIDE - 1)),
            dma((2, SIDE - 1)),
            dma((2,)),
            dma((2,)),
        ],
        compiler_params=pltpu.CompilerParams(
            collective_id=0, has_side_effects=True, vmem_limit_bytes=60 * 1024 * 1024
        ),
        name="expert_steps",
    )(leaving, adopt, routes, gates, tokens, cotangent, w_up, w_down, m_up, v_up, m_down, v_down)


def on_device(
    tokens, cotangent, gates, routes, w_up, w_down, m_up, v_up, m_down, v_down, leaving, tile_owner
):
    experts = lax.axis_size("expert")
    tok_count = tokens.shape[0]
    slot_ids = jnp.arange(experts, dtype=jnp.int32)
    adopt = jnp.sum(
        jnp.where(tile_owner[None, :] == slot_ids[:, None], slot_ids[None, :], 0), axis=1
    )
    outs = expert_steps(
        leaving.reshape(1, 1),
        adopt,
        routes.reshape(1, tok_count),
        gates.reshape(1, tok_count),
        tokens,
        cotangent,
        w_up[0],
        w_down[0],
        m_up[0],
        v_up[0],
        m_down[0],
        v_down[0],
    )
    return tuple(out[None] for out in outs)


def solution(mesh):
    placed = (
        P(("dp", "expert"), None),
        P(("dp", "expert"), None),
        P(("dp", "expert"), None),
        P(("dp", "expert"), None),
        P("expert", None, "dp"),
        P("expert", "dp", None),
        P("expert", None, "dp"),
        P("expert", None, "dp"),
        P("expert", "dp", None),
        P("expert", "dp", None),
        P(),
        P(),
    )
    return jax.shard_map(
        on_device,
        mesh=mesh,
        in_specs=placed,
        out_specs=(
            P("expert", None, "dp"),
            P("expert", "dp", None),
            P("expert", None, "dp"),
            P("expert", None, "dp"),
        ),
        check_vma=False,
    )
```

```python
import functools

import jax
import jax.numpy as jnp
from jax import lax
from jax.experimental import pallas as pl
from jax.experimental.pallas import tpu as pltpu
from jax.sharding import PartitionSpec as P

BETA_ONE = 0.9
BETA_TWO = 0.95
EPSILON = 1e-08

MESH = pl.DeviceIdType.MESH
F32 = jnp.float32
BF16 = jnp.bfloat16

SLOTS = 5
COLS = 16
SIDE = 4
HALF = 4
RING = 8
PARTS = 4
WIDTH = 256
MSG = PARTS * 2 * SLOTS
UNIT = COLS * SLOTS
ALL = COLS * MSG


def mul_t(a, b):
    return lax.dot_general(a, b, (((1,), (1,)), ((), ())), preferred_element_type=F32)


def mul(a, b):
    return lax.dot_general(a, b, (((1,), (0,)), ((), ())), preferred_element_type=F32)


def adam_step(gradient, moment_one, moment_two):
    new_one = BETA_ONE * moment_one.astype(F32) + (1.0 - BETA_ONE) * gradient
    new_two = BETA_TWO * moment_two.astype(F32) + (1.0 - BETA_TWO) * gradient * gradient
    return new_one / (jnp.sqrt(new_two) + EPSILON)


def kernel(
    leaving_ref, adopt_ref, routes_ref, gates_ref, tok_hbm, cot_hbm, wup_hbm, wdn_hbm, mup_hbm, vup_hbm, mdn_hbm, vdn_hbm,
    sup_hbm, sdn_hbm, aup_ref, adn_ref,
    tok, cot, wup, wdn, wup_ward, wdn_ward, mup, vup, mdn, vdn, sup, sdn,
    pick, unpick, packed, landed, own, other, transit, gup, gdn, pg_out, pg_in, gd_out, gd_in,
    leave_up, leave_dn, by_tile, tiles, hop, got, summed, fin, last,
    load_sem, out_sem, plane_send, plane_recv, plane_self,
    chain_send, chain_recv, other_send, transit_send, transit_recv, mate_send, mate_recv,
    ward_send, ward_recv, pg_send, pg_recv, gd_send, gd_recv, hop_send, hop_recv, ring_send, ring_recv, fin_send, fin_recv, last_send, last_recv,
):
    chunks = packed.shape[0]
    half_width = tok.shape[1] // 2
    dp = lax.axis_index("dp")
    ex = lax.axis_index("expert")
    core = lax.rem(dp, 2)
    pos = dp // 2
    zhi = lax.rem(ex, 2)
    col = ex // 2
    cy, cx = col // SIDE, lax.rem(col, SIDE)
    z = zhi * HALF + pos
    me_other = 1 - zhi

    def at_z(z_to):
        return ((z_to % HALF) * 2 + core, col * 2 + z_to // HALF)

    znext, zprev = lax.rem(z + 1, RING), lax.rem(z + RING - 1, RING)
    mate = (pos * 2 + (1 - core), ex)

    def peer_col(i):
        return lax.rem(cy + i // SIDE, SIDE) * SIDE + lax.rem(cx + i % SIDE, SIDE)

    barrier = pltpu.get_barrier_semaphore()
    for i in range(1, COLS):
        pl.semaphore_signal(
            barrier, inc=1, device_id=(dp, peer_col(i) * 2 + zhi), device_id_type=MESH
        )
    twin = (dp, col * 2 + me_other)
    for who in (at_z(znext), at_z(zprev), mate, twin):
        pl.semaphore_signal(barrier, inc=1, device_id=who, device_id_type=MESH)

    loads = [
        pltpu.make_async_copy(src, dst, load_sem.at[i])
        for i, (src, dst) in enumerate(
            (
                (tok_hbm, tok),
                (cot_hbm, cot),
                (wup_hbm, wup),
                (wdn_hbm, wdn),
                (mup_hbm, mup),
                (vup_hbm, vup),
                (mdn_hbm, mdn),
                (vdn_hbm, vdn),
            )
        )
    ]
    for load in loads:
        load.start()

    count = tok.shape[0]
    routes = routes_ref[...]
    expert_ids = lax.broadcasted_iota(jnp.int32, (2 * COLS, count), 0)
    member = (expert_ids == routes).astype(F32)
    before = (
        lax.broadcasted_iota(jnp.int32, (count, count), 0)
        < lax.broadcasted_iota(jnp.int32, (count, count), 1)
    ).astype(BF16)
    rank = jnp.sum(member * mul(member.astype(BF16), before), axis=0, keepdims=True)
    place = (routes >> 1) * MSG + (routes & 1) * SLOTS + rank.astype(jnp.int32)
    eye = lax.broadcasted_iota(jnp.int32, (count, count), 0) == lax.broadcasted_iota(
        jnp.int32, (count, count), 1
    )
    gates = jnp.sum(
        jnp.where(eye, jnp.broadcast_to(gates_ref[...], (count, count)), 0.0), axis=1, keepdims=True
    )
    target = lax.broadcasted_iota(jnp.int32, (ALL, count), 0)
    for part in range(PARTS):
        pick[:, part * count : (part + 1) * count] = (target == place + part * 2 * SLOTS).astype(
            F32
        ).astype(BF16)

    pl.semaphore_wait(barrier, COLS - 1 + 4)

    upper = pos >= 2
    edge = (pos == 0) | (pos == HALF - 1)
    inner = jnp.logical_not(edge)
    out_sign = jnp.where(upper, 1, -1)
    z_out = lax.rem(z + RING + out_sign, RING)
    z_in = lax.rem(z + RING - out_sign, RING)

    def ward_weights(i):
        src, dst = ((wup_hbm, wup_ward), (wdn_hbm, wdn_ward))[i]
        return pltpu.make_async_remote_copy(
            src_ref=src,
            dst_ref=dst,
            send_sem=ward_send.at[i],
            recv_sem=ward_recv.at[i],
            device_id=at_z(z_in),
            device_id_type=MESH,
        )

    @pl.when(edge)
    def _():
        for i in range(2):
            ward_weights(i).start()

    loads[0].wait()
    loads[1].wait()

    def lanes(chunk, high):
        return pl.ds(pl.multiple_of(high * half_width + chunk * WIDTH, 128), WIDTH)

    def plane_copy(chunk, i):
        to = peer_col(i)
        return pltpu.make_async_remote_copy(
            src_ref=packed.at[chunk, to],
            dst_ref=landed.at[chunk, col],
            send_sem=plane_send.at[chunk, i],
            recv_sem=plane_recv.at[chunk, i],
            device_id=(dp, to * 2 + zhi),
            device_id_type=MESH,
        )

    def plane_keep(chunk):
        return pltpu.make_async_copy(
            packed.at[chunk, col], landed.at[chunk, col], plane_self.at[chunk]
        )

    @pl.loop(0, chunks)
    def _(chunk):
        both = [tok[:, lanes(chunk, h)] for h in range(2)]
        both += [
            (gates * cot[:, lanes(chunk, h)].astype(F32)).astype(BF16) for h in range(2)
        ]
        rows = mul(pick[...], jnp.concatenate(both, axis=0))
        packed[chunk] = rows.reshape(COLS, MSG, WIDTH).astype(BF16)
        plane_keep(chunk).start()

        @pl.loop(1, COLS)
        def _(i):
            plane_copy(chunk, i).start()

    line = lax.broadcasted_iota(jnp.int32, (UNIT, ALL), 0)
    source = lax.broadcasted_iota(jnp.int32, (UNIT, ALL), 1)
    fifth = (line * 205) >> 10
    base = fifth * MSG + (line - fifth * SLOTS)
    for part in range(PARTS):
        for which, half in ((0, zhi), (1, me_other)):
            start = (part * 2 + which) * UNIT
            unpick[start : start + UNIT, :] = (
                (source == base + (part * 2 * SLOTS + half * SLOTS)).astype(F32).astype(BF16)
            )

    gup[...] = jnp.zeros_like(gup)
    gdn[...] = jnp.zeros_like(gdn)

    def chain_full(slot, chunk, sem):
        return pltpu.make_async_remote_copy(
            src_ref=own.at[slot, core, chunk],
            dst_ref=own.at[slot, core, chunk],
            send_sem=chain_send.at[sem, slot, chunk],
            recv_sem=chain_recv.at[slot, chunk],
            device_id=at_z(z_in),
            device_id_type=MESH,
        )

    def chain_thin(slot, chunk, sem):
        return pltpu.make_async_remote_copy(
            src_ref=own.at[slot, core, chunk, 0],
            dst_ref=own.at[slot, core, chunk, 0],
            send_sem=chain_send.at[sem, slot, chunk],
            recv_sem=chain_recv.at[slot, chunk],
            device_id=at_z(z_out),
            device_id_type=MESH,
        )

    def hand_full(slot, chunk):
        return pltpu.make_async_remote_copy(
            src_ref=own.at[slot, core, chunk],
            dst_ref=own.at[slot, core, chunk],
            send_sem=mate_send.at[slot, chunk],
            recv_sem=mate_recv.at[slot, chunk],
            device_id=mate,
            device_id_type=MESH,
        )

    def hand_thin(slot, chunk):
        return pltpu.make_async_remote_copy(
            src_ref=own.at[slot, core, chunk, 0],
            dst_ref=own.at[slot, core, chunk, 0],
            send_sem=mate_send.at[slot, chunk],
            recv_sem=mate_recv.at[slot, chunk],
            device_id=mate,
            device_id_type=MESH,
        )

    def other_inner(chunk):
        return pltpu.make_async_remote_copy(
            src_ref=other.at[chunk],
            dst_ref=transit.at[chunk],
            send_sem=other_send.at[chunk],
            recv_sem=transit_recv.at[chunk],
            device_id=at_z(z_out),
            device_id_type=MESH,
        )

    def other_edge(chunk):
        return pltpu.make_async_remote_copy(
            src_ref=other.at[chunk],
            dst_ref=own.at[z, core, chunk],
            send_sem=other_send.at[chunk],
            recv_sem=chain_recv.at[z, chunk],
            device_id=at_z(z_out),
            device_id_type=MESH,
        )

    def transit_edge(chunk):
        return pltpu.make_async_remote_copy(
            src_ref=transit.at[chunk],
            dst_ref=own.at[z_in, core, chunk],
            send_sem=transit_send.at[chunk],
            recv_sem=chain_recv.at[z_in, chunk],
            device_id=at_z(z_out),
            device_id_type=MESH,
        )

    def pg_copy(slot):
        return pltpu.make_async_remote_copy(
            src_ref=pg_out.at[slot],
            dst_ref=pg_in.at[slot],
            send_sem=pg_send.at[slot],
            recv_sem=pg_recv.at[slot],
            device_id=at_z(z_out),
            device_id_type=MESH,
        )

    def gd_copy(b):
        return pltpu.make_async_remote_copy(
            src_ref=gd_out.at[b],
            dst_ref=gd_in.at[b],
            send_sem=gd_send.at[b],
            recv_sem=gd_recv.at[b],
            device_id=at_z(z_out),
            device_id_type=MESH,
        )

    @pl.loop(0, chunks)
    def _(chunk):
        plane_keep(chunk).wait()

        @pl.loop(1, COLS)
        def _(i):
            plane_copy(chunk, i).wait_recv()

        rows = mul(
            unpick[...], landed[chunk].astype(F32).reshape(ALL, WIDTH).astype(BF16)
        ).astype(BF16)
        for part in range(PARTS):
            start = part * 2 * UNIT
            kind, high = part // 2, part % 2
            at = slice(high * WIDTH, (high + 1) * WIDTH)
            own[z, core, chunk, kind, :, at] = rows[start : start + UNIT]
            other[chunk, kind, :, at] = rows[start + UNIT : start + 2 * UNIT]

        @pl.when(edge)
        def _():
            other_edge(chunk).start()
            chain_full(z, chunk, 0).start()
            hand_thin(z, chunk).start()

        @pl.when(inner)
        def _():
            other_inner(chunk).start()
            chain_full(z, chunk, 0).start()
            chain_thin(z, chunk, 1).start()
            hand_full(z, chunk).start()

    for load in loads[2:]:
        load.wait()

    hidden_units = wup.shape[1]

    def pair(slot, chunk, kind, high):
        at = slice(high * WIDTH, (high + 1) * WIDTH)
        return jnp.concatenate(
            [own[slot, 0, chunk, kind, :, at], own[slot, 1, chunk, kind, :, at]], axis=0
        )

    def places():
        for chunk in range(chunks):
            for high in range(2):
                yield chunk, high, high * half_width + chunk * WIDTH

    def terms_inner(slot):
        @pl.loop(0, chunks)
        def _(chunk):
            hand_full(slot, chunk).wait_recv()

        preact = jnp.zeros((2 * UNIT, 2 * hidden_units), F32)
        back = jnp.zeros((2 * UNIT, 2 * hidden_units), F32)
        for chunk, high, at in places():
            here = slice(at, at + WIDTH)
            preact += mul(
                pair(slot, chunk, 0, high),
                jnp.concatenate([wup[here, :], wup_ward[here, :]], axis=1),
            )
            back += mul_t(
                pair(slot, chunk, 1, high),
                jnp.concatenate([wdn[:, here], wdn_ward[:, here]], axis=0),
            )
        squash = jax.nn.sigmoid(preact)
        hidden = preact * squash
        pre_grad = (back * (squash * (1.0 + preact * (1.0 - squash)))).astype(BF16)
        pg_out[slot] = pre_grad[:, hidden_units:]
        hidden = hidden.astype(BF16).astype(F32).T.astype(BF16)
        pre_grad = pre_grad[:, :hidden_units].astype(F32).T.astype(BF16)
        pg_copy(slot).start()
        for chunk, high, at in places():
            here = slice(at, at + WIDTH)
            gdn[:, here] += mul(hidden, pair(slot, chunk, 1, high))
            gup[:, here] += mul(pre_grad, pair(slot, chunk, 0, high))

    def terms_edge(slot):
        @pl.loop(0, chunks)
        def _(chunk):
            hand_thin(slot, chunk).wait_recv()

        pg_copy(slot).wait_recv()
        pre_grad = pg_in[slot].astype(F32).T.astype(BF16)
        for chunk, high, at in places():
            gup[:, at : at + WIDTH] += mul(pre_grad, pair(slot, chunk, 0, high))

    def toward_out(far):
        return lax.rem(z + RING + out_sign * far, RING)

    def relay_out(far, chunk):
        slot = toward_out(far)
        chain_full(slot, chunk, 0).wait_recv()
        chain_full(slot, chunk, 0).start()

        @pl.when(edge)
        def _():
            hand_thin(slot, chunk).start()

        @pl.when(inner)
        def _():
            hand_full(slot, chunk).start()

    def relay_in(far, chunk):
        slot = toward_out(-far)
        chain_full(slot, chunk, 0).wait_recv()
        chain_thin(slot, chunk, 0).start()
        hand_full(slot, chunk).start()

    def edge_unit(i):
        thin = (i == 0) | (lax.rem(i, 2) == 1)
        far = jnp.where(i == 0, 1, (i + 3) // 2)
        return thin, toward_out(jnp.where(thin, -far, i // 2 - 1))

    @pl.when(edge)
    def _():
        @pl.loop(0, chunks)
        def _(chunk):
            other_inner(chunk).wait_recv()
            transit_edge(chunk).start()
            relay_out(1, chunk)

        @pl.loop(0, chunks)
        def _(chunk):
            relay_out(2, chunk)

        @pl.loop(0, RING)
        def _(i):
            thin, slot = edge_unit(i)

            @pl.when(thin)
            def _():
                @pl.loop(0, chunks)
                def _(chunk):
                    chain_thin(slot, chunk, 0).wait_recv()
                    hand_thin(slot, chunk).start()

            terms_edge(slot)

    @pl.when(inner)
    def _():
        @pl.loop(0, chunks)
        def _(chunk):
            relay_in(1, chunk)

        for i in range(2):
            ward_weights(i).wait_recv()

        @pl.loop(1, HALF)
        def _(k):
            @pl.loop(0, chunks)
            def _(chunk):
                relay_out(k, chunk)
                relay_in(k + 1, chunk)
                first = chunk == 2

                @pl.when(first | (chunk == 5))
                def _():
                    terms_inner(toward_out(jnp.where(first, k - 1, -k)))

        @pl.loop(0, 2)
        def _(i):
            terms_inner(toward_out(jnp.where(i == 0, HALF - 1, -HALF)))

        span = gd_out.shape[2]
        for b in range(gd_out.shape[0]):
            gd_out[b] = gdn[hidden_units:, b * span : (b + 1) * span].astype(BF16)
            gd_copy(b).start()

    model_width = tok.shape[1]
    block = 128
    leaves = jnp.broadcast_to(leaving_ref[...], (block, block)) == ex
    ring_at, line_at = (cx, cy), (cy, cx)
    middle = SIDE

    def tile_home(axis, ring_to, line_to):
        to = line_to * SIDE + ring_to if axis == 0 else ring_to * SIDE + line_to
        return (dp, to * 2 + zhi)

    def ring_next(axis, far):
        return lax.rem(ring_at[axis] + far, SIDE)

    def ring_to(axis, side):
        return tile_home(axis, ring_next(axis, 1 if side == 0 else SIDE - 1), line_at[axis])

    def part_of(side):
        return pl.ds(0, middle) if side == 0 else pl.ds(middle, middle)

    def hop_copy(axis, side):
        return pltpu.make_async_remote_copy(
            src_ref=tiles.at[axis, ring_next(axis, 2), part_of(side)],
            dst_ref=hop.at[axis, side],
            send_sem=hop_send.at[axis, side],
            recv_sem=hop_recv.at[axis, side],
            device_id=ring_to(axis, side),
            device_id_type=MESH,
        )

    def ring_copy(axis, side, late):
        part = part_of(side if late else 1 - side)
        return pltpu.make_async_remote_copy(
            src_ref=tiles.at[axis, ring_next(axis, 1 if side == 0 else SIDE - 1), part],
            dst_ref=got.at[axis, side, part],
            send_sem=ring_send.at[axis, side, late],
            recv_sem=ring_recv.at[axis, side, late],
            device_id=ring_to(axis, side),
            device_id_type=MESH,
        )

    def fin_copy(axis, far):
        line_to = lax.rem(line_at[axis] + far, SIDE)
        return pltpu.make_async_remote_copy(
            src_ref=summed.at[axis, pl.ds(line_to * 2, 2)],
            dst_ref=fin.at[axis, far - 1],
            send_sem=fin_send.at[axis, far - 1],
            recv_sem=fin_recv.at[axis, far - 1],
            device_id=tile_home(axis, ring_at[axis], line_to),
            device_id_type=MESH,
        )

    def last_copy(axis):
        return pltpu.make_async_remote_copy(
            src_ref=summed.at[axis, line_at[axis] * 2 + me_other],
            dst_ref=last.at[axis],
            send_sem=last_send.at[axis],
            recv_sem=last_recv.at[axis],
            device_id=twin,
            device_id_type=MESH,
        )

    def sort_tiles(axis, leave):
        rows = tiles.shape[3]
        for tile in range(2 * COLS):
            by_tile[tile] = leave[tile * rows : (tile + 1) * rows, :]

        @pl.loop(0, 2 * COLS)
        def _(owner):
            to = owner // 2
            ty, tx = to // SIDE, lax.rem(to, SIDE)
            r, l = (tx, ty) if axis == 0 else (ty, tx)
            tiles[axis, r, l * 2 + lax.rem(owner, 2)] = by_tile[adopt_ref[owner]]

        for side in range(2):
            hop_copy(axis, side).start()
        for side in range(2):
            ring_copy(axis, side, 0).start()

    @pl.loop(0, model_width // block)
    def _(b):
        at = pl.ds(pl.multiple_of(b * block, block), block)
        step = adam_step(gup[:, at].T, mup[at, :], vup[at, :])
        sup[at, :] = jnp.where(leaves, 0.0, step).astype(BF16)
        leave_up[at, :] = jnp.where(leaves, step, 0.0).astype(BF16)

    out_up = pltpu.make_async_copy(sup, sup_hbm, out_sem.at[0])
    out_up.start()
    sort_tiles(0, leave_up)

    def pass_on(axis):
        for side in range(2):
            hop_copy(axis, side).wait_recv()
            to = ring_next(axis, 1 if side == 0 else SIDE - 1)
            part = part_of(side)
            tiles[axis, to, part] = tiles[axis, to, part] + hop[axis, side]
            ring_copy(axis, side, 1).start()

    pass_on(0)
    span = gd_in.shape[2]

    @pl.loop(0, gd_in.shape[0])
    def _(b):
        @pl.when(edge)
        def _():
            gd_copy(b).wait_recv()
            gdn[0:hidden_units, pl.ds(pl.multiple_of(b * span, block), span)] = gd_in[b].astype(F32)

        @pl.loop(0, span // block)
        def _(i):
            at = pl.ds(pl.multiple_of(b * span + i * block, block), block)
            step = adam_step(gdn[0:hidden_units, at], mdn[:, at], vdn[:, at])
            sdn[:, at] = jnp.where(leaves, 0.0, step).astype(BF16)
            leave_dn[at, :] = jnp.where(leaves, step, 0.0).T.astype(BF16)

    out_dn = pltpu.make_async_copy(sdn, sdn_hbm, out_sem.at[1])
    out_dn.start()
    sort_tiles(1, leave_dn)

    pass_on(1)

    for axis in range(2):
        for side in range(2):
            for late in range(2):
                ring_copy(axis, side, late).wait_recv()
        summed[axis] = tiles[axis, ring_at[axis]] + got[axis, 0] + got[axis, 1]
        for far in range(1, SIDE):
            fin_copy(axis, far).start()

    for axis in range(2):
        for far in range(1, SIDE):
            fin_copy(axis, far).wait_recv()
        mine = pl.ds(line_at[axis] * 2, 2)
        summed[axis, mine] = summed[axis, mine] + fin[axis, 0] + fin[axis, 1] + fin[axis, 2]
        last_copy(axis).start()

    for axis, adopted in ((0, aup_ref), (1, adn_ref)):
        last_copy(axis).wait_recv()
        adopted[...] = summed[axis, line_at[axis] * 2 + zhi] + last[axis]

    for axis in range(2):
        for side in range(2):
            hop_copy(axis, side).wait_send()
            for late in range(2):
                ring_copy(axis, side, late).wait_send()
        for far in range(1, SIDE):
            fin_copy(axis, far).wait_send()
        last_copy(axis).wait_send()

    @pl.loop(0, chunks)
    def _(chunk):
        @pl.loop(1, COLS)
        def _(i):
            plane_copy(chunk, i).wait_send()

        other_inner(chunk).wait_send()
        chain_full(z, chunk, 0).wait_send()

        @pl.when(edge)
        def _():
            transit_edge(chunk).wait_send()
            hand_thin(z, chunk).wait_send()

            @pl.loop(1, 3)
            def _(far):
                chain_full(toward_out(far), chunk, 0).wait_send()
                hand_thin(toward_out(far), chunk).wait_send()

            @pl.loop(1, 6)
            def _(far):
                hand_thin(toward_out(-far), chunk).wait_send()

        @pl.when(inner)
        def _():
            chain_thin(z, chunk, 1).wait_send()
            hand_full(z, chunk).wait_send()

            @pl.loop(1, 4)
            def _(far):
                chain_full(toward_out(far), chunk, 0).wait_send()
                hand_full(toward_out(far), chunk).wait_send()

            @pl.loop(1, 5)
            def _(far):
                chain_thin(toward_out(-far), chunk, 0).wait_send()
                hand_full(toward_out(-far), chunk).wait_send()

    @pl.when(edge)
    def _():
        for i in range(2):
            ward_weights(i).wait_send()

    @pl.when(inner)
    def _():
        @pl.loop(0, RING)
        def _(slot):
            pg_copy(slot).wait_send()

        @pl.loop(0, gd_out.shape[0])
        def _(b):
            gd_copy(b).wait_send()

    out_up.wait()
    out_dn.wait()


def expert_steps(leaving, adopt, routes, gates, tokens, cotangent, w_up, w_down, m_up, v_up, m_down, v_down):
    count, model_width = tokens.shape
    hidden = w_up.shape[1]
    chunks = model_width // 2 // WIDTH
    tile_rows = model_width // adopt.shape[0]
    smem = pl.BlockSpec(memory_space=pltpu.SMEM)
    vmem = pl.BlockSpec(memory_space=pltpu.VMEM)
    anyw = pl.BlockSpec(memory_space=pl.ANY)
    dma = pltpu.SemaphoreType.DMA
    return pl.pallas_call(
        kernel,
        out_shape=(
            jax.ShapeDtypeStruct((model_width, hidden), BF16),
            jax.ShapeDtypeStruct((hidden, model_width), BF16),
            jax.ShapeDtypeStruct((tile_rows, hidden), BF16),
            jax.ShapeDtypeStruct((tile_rows, hidden), BF16),
        ),
        in_specs=[vmem, smem, vmem, vmem] + [anyw] * 8,
        out_specs=(anyw, anyw, vmem, vmem),
        scratch_shapes=[
            pltpu.VMEM((count, model_width), BF16),
            pltpu.VMEM((count, model_width), BF16),
            pltpu.VMEM((model_width, hidden), BF16),
            pltpu.VMEM((hidden, model_width), BF16),
            pltpu.VMEM((model_width, hidden), BF16),
            pltpu.VMEM((hidden, model_width), BF16),
            pltpu.VMEM((model_width, hidden), BF16),
            pltpu.VMEM((model_width, hidden), BF16),
            pltpu.VMEM((hidden, model_width), BF16),
            pltpu.VMEM((hidden, model_width), BF16),
            pltpu.VMEM((model_width, hidden), BF16),
            pltpu.VMEM((hidden, model_width), BF16),
            pltpu.VMEM((ALL, PARTS * count), BF16),
            pltpu.VMEM((PARTS * 2 * UNIT, ALL), BF16),
            pltpu.VMEM((chunks, COLS, MSG, WIDTH), BF16),
            pltpu.VMEM((chunks, COLS, MSG, WIDTH), BF16),
            pltpu.VMEM((RING, 2, chunks, 2, UNIT, 2 * WIDTH), BF16),
            pltpu.VMEM((chunks, 2, UNIT, 2 * WIDTH), BF16),
            pltpu.VMEM((chunks, 2, UNIT, 2 * WIDTH), BF16),
            pltpu.VMEM((hidden, model_width), F32),
            pltpu.VMEM((2 * hidden, model_width), F32),
            pltpu.VMEM((RING, 2 * UNIT, hidden), BF16),
            pltpu.VMEM((RING, 2 * UNIT, hidden), BF16),
            pltpu.VMEM((7, hidden, model_width // 7), BF16),
            pltpu.VMEM((7, hidden, model_width // 7), BF16),
            pltpu.VMEM((model_width, hidden), BF16),
            pltpu.VMEM((model_width, hidden), BF16),
            pltpu.VMEM((2 * COLS, tile_rows, hidden), BF16),
            pltpu.VMEM((2, SIDE, 2 * SIDE, tile_rows, hidden), BF16),
            pltpu.VMEM((2, 2, SIDE, tile_rows, hidden), BF16),
            pltpu.VMEM((2, 2, 2 * SIDE, tile_rows, hidden), BF16),
            pltpu.VMEM((2, 2 * SIDE, tile_rows, hidden), BF16),
            pltpu.VMEM((2, SIDE - 1, 2, tile_rows, hidden), BF16),
            pltpu.VMEM((2, tile_rows, hidden), BF16),
            dma((8,)),
            dma((2,)),
            dma((chunks, COLS)),
            dma((chunks, COLS)),
            dma((chunks,)),
            dma((2, RING, chunks)),
            dma((RING, chunks)),
            dma((chunks,)),
            dma((chunks,)),
            dma((chunks,)),
            dma((RING, chunks)),
            dma((RING, chunks)),
            dma((2,)),
            dma((2,)),
            dma((RING,)),
            dma((RING,)),
            dma((7,)),
            dma((7,)),
            dma((2, 2)),
            dma((2, 2)),
            dma((2, 2, 2)),
            dma((2, 2, 2)),
            dma((2, SIDE - 1)),
            dma((2, SIDE - 1)),
            dma((2,)),
            dma((2,)),
        ],
        compiler_params=pltpu.CompilerParams(
            collective_id=0, has_side_effects=True, vmem_limit_bytes=62 * 1024 * 1024
        ),
        name="expert_steps",
    )(leaving, adopt, routes, gates, tokens, cotangent, w_up, w_down, m_up, v_up, m_down, v_down)


def on_device(
    tokens, cotangent, gates, routes, w_up, w_down, m_up, v_up, m_down, v_down, leaving, tile_owner
):
    experts = lax.axis_size("expert")
    tok_count = tokens.shape[0]
    slot_ids = jnp.arange(experts, dtype=jnp.int32)
    adopt = jnp.sum(
        jnp.where(tile_owner[None, :] == slot_ids[:, None], slot_ids[None, :], 0), axis=1
    )
    outs = expert_steps(
        leaving.reshape(1, 1),
        adopt,
        routes.reshape(1, tok_count),
        gates.reshape(1, tok_count),
        tokens,
        cotangent,
        w_up[0],
        w_down[0],
        m_up[0],
        v_up[0],
        m_down[0],
        v_down[0],
    )
    return tuple(out[None] for out in outs)


def solution(mesh):
    placed = (
        P(("dp", "expert"), None),
        P(("dp", "expert"), None),
        P(("dp", "expert"), None),
        P(("dp", "expert"), None),
        P("expert", None, "dp"),
        P("expert", "dp", None),
        P("expert", None, "dp"),
        P("expert", None, "dp"),
        P("expert", "dp", None),
        P("expert", "dp", None),
        P(),
        P(),
    )
    return jax.shard_map(
        on_device,
        mesh=mesh,
        in_specs=placed,
        out_specs=(
            P("expert", None, "dp"),
            P("expert", "dp", None),
            P("expert", None, "dp"),
            P("expert", None, "dp"),
        ),
        check_vma=False,
    )
```

```python
import functools

import jax
import jax.numpy as jnp
from jax import lax
from jax.experimental import pallas as pl
from jax.experimental.pallas import tpu as pltpu
from jax.sharding import PartitionSpec as P

BETA_ONE = 0.9
BETA_TWO = 0.95
EPSILON = 1e-08

MESH = pl.DeviceIdType.MESH
F32 = jnp.float32
BF16 = jnp.bfloat16

SLOTS = 5
COLS = 16
SIDE = 4
HALF = 4
RING = 8
PARTS = 4
WIDTH = 256
MSG = PARTS * 2 * SLOTS
UNIT = COLS * SLOTS
ALL = COLS * MSG
LAG = 3


def mul_t(a, b):
    return lax.dot_general(a, b, (((1,), (1,)), ((), ())), preferred_element_type=F32)


def mul(a, b):
    return lax.dot_general(a, b, (((1,), (0,)), ((), ())), preferred_element_type=F32)


def adam_step(gradient, moment_one, moment_two):
    new_one = BETA_ONE * moment_one.astype(F32) + (1.0 - BETA_ONE) * gradient
    new_two = BETA_TWO * moment_two.astype(F32) + (1.0 - BETA_TWO) * gradient * gradient
    return new_one / (jnp.sqrt(new_two) + EPSILON)


def kernel(
    leaving_ref, adopt_ref, routes_ref, gates_ref, tok_hbm, cot_hbm, wup_hbm, wdn_hbm, mup_hbm, vup_hbm, mdn_hbm, vdn_hbm,
    sup_hbm, sdn_hbm, aup_ref, adn_ref,
    tok, cot, wup, wdn, wup_ward, wdn_ward, mup, vup, mdn, vdn, sup, sdn,
    pick, unpick, packed, landed, own, other, transit, gup, gdn, pg_out, pg_in, gd_out, gd_in,
    leave_up, leave_dn, by_tile, tiles, hop, got, summed, fin, last,
    load_sem, out_sem, plane_send, plane_recv, plane_self,
    chain_send, chain_recv, other_send, transit_send, transit_recv, mate_send, mate_recv,
    ward_send, ward_recv, pg_send, pg_recv, gd_send, gd_recv, hop_send, hop_recv, ring_send, ring_recv, fin_send, fin_recv, last_send, last_recv,
):
    chunks = packed.shape[0]
    half_width = tok.shape[1] // 2
    dp = lax.axis_index("dp")
    ex = lax.axis_index("expert")
    core = lax.rem(dp, 2)
    pos = dp // 2
    zhi = lax.rem(ex, 2)
    col = ex // 2
    cy, cx = col // SIDE, lax.rem(col, SIDE)
    z = zhi * HALF + pos
    me_other = 1 - zhi

    def at_z(z_to):
        return ((z_to % HALF) * 2 + core, col * 2 + z_to // HALF)

    znext, zprev = lax.rem(z + 1, RING), lax.rem(z + RING - 1, RING)
    mate = (pos * 2 + (1 - core), ex)

    def peer_col(i):
        return lax.rem(cy + i // SIDE, SIDE) * SIDE + lax.rem(cx + i % SIDE, SIDE)

    barrier = pltpu.get_barrier_semaphore()
    for i in range(1, COLS):
        pl.semaphore_signal(
            barrier, inc=1, device_id=(dp, peer_col(i) * 2 + zhi), device_id_type=MESH
        )
    twin = (dp, col * 2 + me_other)
    for who in (at_z(znext), at_z(zprev), mate, twin):
        pl.semaphore_signal(barrier, inc=1, device_id=who, device_id_type=MESH)

    loads = [
        pltpu.make_async_copy(src, dst, load_sem.at[i])
        for i, (src, dst) in enumerate(
            (
                (tok_hbm, tok),
                (cot_hbm, cot),
                (wup_hbm, wup),
                (wdn_hbm, wdn),
                (mup_hbm, mup),
                (vup_hbm, vup),
                (mdn_hbm, mdn),
                (vdn_hbm, vdn),
            )
        )
    ]
    for load in loads:
        load.start()

    count = tok.shape[0]
    routes = routes_ref[...]
    expert_ids = lax.broadcasted_iota(jnp.int32, (2 * COLS, count), 0)
    member = (expert_ids == routes).astype(F32)
    before = (
        lax.broadcasted_iota(jnp.int32, (count, count), 0)
        < lax.broadcasted_iota(jnp.int32, (count, count), 1)
    ).astype(BF16)
    rank = jnp.sum(member * mul(member.astype(BF16), before), axis=0, keepdims=True)
    place = (routes >> 1) * MSG + (routes & 1) * SLOTS + rank.astype(jnp.int32)
    eye = lax.broadcasted_iota(jnp.int32, (count, count), 0) == lax.broadcasted_iota(
        jnp.int32, (count, count), 1
    )
    gates = jnp.sum(
        jnp.where(eye, jnp.broadcast_to(gates_ref[...], (count, count)), 0.0), axis=1, keepdims=True
    )
    target = lax.broadcasted_iota(jnp.int32, (ALL, count), 0)
    for part in range(PARTS):
        pick[:, part * count : (part + 1) * count] = (target == place + part * 2 * SLOTS).astype(
            F32
        ).astype(BF16)

    pl.semaphore_wait(barrier, COLS - 1 + 4)

    upper = pos >= 2
    edge = (pos == 0) | (pos == HALF - 1)
    inner = jnp.logical_not(edge)
    out_sign = jnp.where(upper, 1, -1)
    z_out = lax.rem(z + RING + out_sign, RING)
    z_in = lax.rem(z + RING - out_sign, RING)

    def ward_weights(i):
        src, dst = ((wup_hbm, wup_ward), (wdn_hbm, wdn_ward))[i]
        return pltpu.make_async_remote_copy(
            src_ref=src,
            dst_ref=dst,
            send_sem=ward_send.at[i],
            recv_sem=ward_recv.at[i],
            device_id=at_z(z_in),
            device_id_type=MESH,
        )

    @pl.when(edge)
    def _():
        for i in range(2):
            ward_weights(i).start()

    loads[0].wait()
    loads[1].wait()

    def lanes(chunk, high):
        return pl.ds(pl.multiple_of(high * half_width + chunk * WIDTH, 128), WIDTH)

    def plane_copy(chunk, i):
        to = peer_col(i)
        return pltpu.make_async_remote_copy(
            src_ref=packed.at[chunk, to],
            dst_ref=landed.at[chunk, col],
            send_sem=plane_send.at[chunk, i],
            recv_sem=plane_recv.at[chunk, i],
            device_id=(dp, to * 2 + zhi),
            device_id_type=MESH,
        )

    def plane_keep(chunk):
        return pltpu.make_async_copy(
            packed.at[chunk, col], landed.at[chunk, col], plane_self.at[chunk]
        )

    @pl.loop(0, chunks)
    def _(chunk):
        both = [tok[:, lanes(chunk, h)] for h in range(2)]
        both += [
            (gates * cot[:, lanes(chunk, h)].astype(F32)).astype(BF16) for h in range(2)
        ]
        rows = mul(pick[...], jnp.concatenate(both, axis=0))
        packed[chunk] = rows.reshape(COLS, MSG, WIDTH).astype(BF16)
        plane_keep(chunk).start()

        @pl.loop(1, COLS)
        def _(i):
            plane_copy(chunk, i).start()

    line = lax.broadcasted_iota(jnp.int32, (UNIT, ALL), 0)
    source = lax.broadcasted_iota(jnp.int32, (UNIT, ALL), 1)
    fifth = (line * 205) >> 10
    base = fifth * MSG + (line - fifth * SLOTS)
    for part in range(PARTS):
        for which, half in ((0, zhi), (1, me_other)):
            start = (part * 2 + which) * UNIT
            unpick[start : start + UNIT, :] = (
                (source == base + (part * 2 * SLOTS + half * SLOTS)).astype(F32).astype(BF16)
            )

    gup[...] = jnp.zeros_like(gup)
    gdn[...] = jnp.zeros_like(gdn)

    def chain_full(slot, chunk, sem):
        return pltpu.make_async_remote_copy(
            src_ref=own.at[slot, core, chunk],
            dst_ref=own.at[slot, core, chunk],
            send_sem=chain_send.at[sem, slot, chunk],
            recv_sem=chain_recv.at[slot, chunk],
            device_id=at_z(z_in),
            device_id_type=MESH,
        )

    def chain_thin(slot, chunk, sem):
        return pltpu.make_async_remote_copy(
            src_ref=own.at[slot, core, chunk, 0],
            dst_ref=own.at[slot, core, chunk, 0],
            send_sem=chain_send.at[sem, slot, chunk],
            recv_sem=chain_recv.at[slot, chunk],
            device_id=at_z(z_out),
            device_id_type=MESH,
        )

    def hand_full(slot, chunk):
        return pltpu.make_async_remote_copy(
            src_ref=own.at[slot, core, chunk],
            dst_ref=own.at[slot, core, chunk],
            send_sem=mate_send.at[slot, chunk],
            recv_sem=mate_recv.at[slot, chunk],
            device_id=mate,
            device_id_type=MESH,
        )

    def hand_thin(slot, chunk):
        return pltpu.make_async_remote_copy(
            src_ref=own.at[slot, core, chunk, 0],
            dst_ref=own.at[slot, core, chunk, 0],
            send_sem=mate_send.at[slot, chunk],
            recv_sem=mate_recv.at[slot, chunk],
            device_id=mate,
            device_id_type=MESH,
        )

    def other_inner(chunk):
        return pltpu.make_async_remote_copy(
            src_ref=other.at[chunk],
            dst_ref=transit.at[chunk],
            send_sem=other_send.at[chunk],
            recv_sem=transit_recv.at[chunk],
            device_id=at_z(z_out),
            device_id_type=MESH,
        )

    def other_edge(chunk):
        return pltpu.make_async_remote_copy(
            src_ref=other.at[chunk],
            dst_ref=own.at[z, core, chunk],
            send_sem=other_send.at[chunk],
            recv_sem=chain_recv.at[z, chunk],
            device_id=at_z(z_out),
            device_id_type=MESH,
        )

    def transit_edge(chunk):
        return pltpu.make_async_remote_copy(
            src_ref=transit.at[chunk],
            dst_ref=own.at[z_in, core, chunk],
            send_sem=transit_send.at[chunk],
            recv_sem=chain_recv.at[z_in, chunk],
            device_id=at_z(z_out),
            device_id_type=MESH,
        )

    def pg_copy(slot):
        return pltpu.make_async_remote_copy(
            src_ref=pg_out.at[slot],
            dst_ref=pg_in.at[slot],
            send_sem=pg_send.at[slot],
            recv_sem=pg_recv.at[slot],
            device_id=at_z(z_out),
            device_id_type=MESH,
        )

    def gd_copy(b):
        return pltpu.make_async_remote_copy(
            src_ref=gd_out.at[b],
            dst_ref=gd_in.at[b],
            send_sem=gd_send.at[b],
            recv_sem=gd_recv.at[b],
            device_id=at_z(z_out),
            device_id_type=MESH,
        )

    @pl.loop(0, chunks)
    def _(chunk):
        plane_keep(chunk).wait()

        @pl.loop(1, COLS)
        def _(i):
            plane_copy(chunk, i).wait_recv()

        rows = mul(
            unpick[...], landed[chunk].astype(F32).reshape(ALL, WIDTH).astype(BF16)
        ).astype(BF16)
        for part in range(PARTS):
            start = part * 2 * UNIT
            kind, high = part // 2, part % 2
            at = slice(high * WIDTH, (high + 1) * WIDTH)
            own[z, core, chunk, kind, :, at] = rows[start : start + UNIT]
            other[chunk, kind, :, at] = rows[start + UNIT : start + 2 * UNIT]

        @pl.when(edge)
        def _():
            other_edge(chunk).start()
            chain_full(z, chunk, 0).start()
            hand_thin(z, chunk).start()

        @pl.when(inner)
        def _():
            other_inner(chunk).start()
            chain_full(z, chunk, 0).start()
            chain_thin(z, chunk, 1).start()
            hand_full(z, chunk).start()

    for load in loads[2:]:
        load.wait()

    hidden_units = wup.shape[1]

    def pair(slot, chunk, kind, high):
        at = slice(high * WIDTH, (high + 1) * WIDTH)
        return jnp.concatenate(
            [own[slot, 0, chunk, kind, :, at], own[slot, 1, chunk, kind, :, at]], axis=0
        )

    def places():
        for chunk in range(chunks):
            for high in range(2):
                yield chunk, high, high * half_width + chunk * WIDTH

    def terms_inner(slot):
        @pl.loop(0, chunks)
        def _(chunk):
            hand_full(slot, chunk).wait_recv()

        preact = jnp.zeros((2 * UNIT, 2 * hidden_units), F32)
        back = jnp.zeros((2 * UNIT, 2 * hidden_units), F32)
        for chunk, high, at in places():
            here = slice(at, at + WIDTH)
            preact += mul(
                pair(slot, chunk, 0, high),
                jnp.concatenate([wup[here, :], wup_ward[here, :]], axis=1),
            )
            back += mul_t(
                pair(slot, chunk, 1, high),
                jnp.concatenate([wdn[:, here], wdn_ward[:, here]], axis=0),
            )
        squash = jax.nn.sigmoid(preact)
        hidden = preact * squash
        pre_grad = (back * (squash * (1.0 + preact * (1.0 - squash)))).astype(BF16)
        pg_out[slot] = pre_grad[:, hidden_units:]
        hidden = hidden.astype(BF16).astype(F32).T.astype(BF16)
        pre_grad = pre_grad[:, :hidden_units].astype(F32).T.astype(BF16)
        pg_copy(slot).start()
        for chunk, high, at in places():
            here = slice(at, at + WIDTH)
            gdn[:, here] += mul(hidden, pair(slot, chunk, 1, high))
            gup[:, here] += mul(pre_grad, pair(slot, chunk, 0, high))

    def terms_edge(slot):
        @pl.loop(0, chunks)
        def _(chunk):
            hand_thin(slot, chunk).wait_recv()

        pg_copy(slot).wait_recv()
        pre_grad = pg_in[slot].astype(F32).T.astype(BF16)
        for chunk, high, at in places():
            gup[:, at : at + WIDTH] += mul(pre_grad, pair(slot, chunk, 0, high))

    def toward_out(far):
        return lax.rem(z + RING + out_sign * far, RING)

    def relay_out(far, chunk):
        slot = toward_out(far)
        chain_full(slot, chunk, 0).wait_recv()
        chain_full(slot, chunk, 0).start()

        @pl.when(edge)
        def _():
            hand_thin(slot, chunk).start()

        @pl.when(inner)
        def _():
            hand_full(slot, chunk).start()

    def relay_in(far, chunk):
        slot = toward_out(-far)
        chain_full(slot, chunk, 0).wait_recv()
        chain_thin(slot, chunk, 0).start()
        hand_full(slot, chunk).start()

    def edge_unit(i):
        thin = (i == 0) | (lax.rem(i, 2) == 1)
        far = jnp.where(i == 0, 1, (i + 3) // 2)
        return thin, toward_out(jnp.where(thin, -far, i // 2 - 1))

    @pl.when(edge)
    def _():
        @pl.loop(0, chunks)
        def _(chunk):
            other_inner(chunk).wait_recv()
            transit_edge(chunk).start()
            relay_out(1, chunk)

        @pl.loop(0, chunks)
        def _(chunk):
            relay_out(2, chunk)

        @pl.loop(0, RING)
        def _(i):
            thin, slot = edge_unit(i)

            @pl.when(thin)
            def _():
                @pl.loop(0, chunks)
                def _(chunk):
                    chain_thin(slot, chunk, 0).wait_recv()
                    hand_thin(slot, chunk).start()

            terms_edge(slot)

    @pl.when(inner)
    def _():
        @pl.loop(0, chunks)
        def _(chunk):
            relay_in(1, chunk)

        for i in range(2):
            ward_weights(i).wait_recv()

        def relay_in_at(item):
            relay_in(item // chunks + 1, lax.rem(item, chunks))

        steps = (HALF - 1) * chunks

        @pl.loop(0, steps)
        def _(item):
            relay_out(item // chunks + 1, lax.rem(item, chunks))

            @pl.when(item >= LAG)
            def _():
                relay_in_at(item + chunks - LAG)

            @pl.when(lax.rem(item, 3) == 2)
            def _():
                turn = item // 3
                terms_inner(
                    toward_out(jnp.where(lax.rem(turn, 2) == 0, turn // 2, -((turn + 1) // 2)))
                )

        @pl.loop(0, LAG)
        def _(i):
            relay_in_at(steps + chunks - LAG + i)

        terms_inner(toward_out(-HALF))

        span = gd_out.shape[2]
        for b in range(gd_out.shape[0]):
            gd_out[b] = gdn[hidden_units:, b * span : (b + 1) * span].astype(BF16)
            gd_copy(b).start()

    model_width = tok.shape[1]
    block = 128
    leaves = jnp.broadcast_to(leaving_ref[...], (block, block)) == ex
    ring_at, line_at = (cx, cy), (cy, cx)
    middle = SIDE

    def tile_home(axis, ring_to, line_to):
        to = line_to * SIDE + ring_to if axis == 0 else ring_to * SIDE + line_to
        return (dp, to * 2 + zhi)

    def ring_next(axis, far):
        return lax.rem(ring_at[axis] + far, SIDE)

    def ring_to(axis, side):
        return tile_home(axis, ring_next(axis, 1 if side == 0 else SIDE - 1), line_at[axis])

    def part_of(side):
        return pl.ds(0, middle) if side == 0 else pl.ds(middle, middle)

    def hop_copy(axis, side):
        return pltpu.make_async_remote_copy(
            src_ref=tiles.at[axis, ring_next(axis, 2), part_of(side)],
            dst_ref=hop.at[axis, side],
            send_sem=hop_send.at[axis, side],
            recv_sem=hop_recv.at[axis, side],
            device_id=ring_to(axis, side),
            device_id_type=MESH,
        )

    def ring_copy(axis, side, late):
        part = part_of(side if late else 1 - side)
        return pltpu.make_async_remote_copy(
            src_ref=tiles.at[axis, ring_next(axis, 1 if side == 0 else SIDE - 1), part],
            dst_ref=got.at[axis, side, part],
            send_sem=ring_send.at[axis, side, late],
            recv_sem=ring_recv.at[axis, side, late],
            device_id=ring_to(axis, side),
            device_id_type=MESH,
        )

    def fin_copy(axis, far):
        line_to = lax.rem(line_at[axis] + far, SIDE)
        return pltpu.make_async_remote_copy(
            src_ref=summed.at[axis, pl.ds(line_to * 2, 2)],
            dst_ref=fin.at[axis, far - 1],
            send_sem=fin_send.at[axis, far - 1],
            recv_sem=fin_recv.at[axis, far - 1],
            device_id=tile_home(axis, ring_at[axis], line_to),
            device_id_type=MESH,
        )

    def last_copy(axis):
        return pltpu.make_async_remote_copy(
            src_ref=summed.at[axis, line_at[axis] * 2 + me_other],
            dst_ref=last.at[axis],
            send_sem=last_send.at[axis],
            recv_sem=last_recv.at[axis],
            device_id=twin,
            device_id_type=MESH,
        )

    def sort_tiles(axis, leave):
        rows = tiles.shape[3]
        for tile in range(2 * COLS):
            by_tile[tile] = leave[tile * rows : (tile + 1) * rows, :]

        @pl.loop(0, 2 * COLS)
        def _(owner):
            to = owner // 2
            ty, tx = to // SIDE, lax.rem(to, SIDE)
            r, l = (tx, ty) if axis == 0 else (ty, tx)
            tiles[axis, r, l * 2 + lax.rem(owner, 2)] = by_tile[adopt_ref[owner]]

        for side in range(2):
            hop_copy(axis, side).start()
        for side in range(2):
            ring_copy(axis, side, 0).start()

    @pl.loop(0, model_width // block)
    def _(b):
        at = pl.ds(pl.multiple_of(b * block, block), block)
        step = adam_step(gup[:, at].T, mup[at, :], vup[at, :])
        sup[at, :] = jnp.where(leaves, 0.0, step).astype(BF16)
        leave_up[at, :] = jnp.where(leaves, step, 0.0).astype(BF16)

    out_up = pltpu.make_async_copy(sup, sup_hbm, out_sem.at[0])
    out_up.start()
    sort_tiles(0, leave_up)

    def pass_on(axis):
        for side in range(2):
            hop_copy(axis, side).wait_recv()
            to = ring_next(axis, 1 if side == 0 else SIDE - 1)
            part = part_of(side)
            tiles[axis, to, part] = tiles[axis, to, part] + hop[axis, side]
            ring_copy(axis, side, 1).start()

    pass_on(0)
    span = gd_in.shape[2]

    @pl.loop(0, gd_in.shape[0])
    def _(b):
        @pl.when(edge)
        def _():
            gd_copy(b).wait_recv()
            gdn[0:hidden_units, pl.ds(pl.multiple_of(b * span, block), span)] = gd_in[b].astype(F32)

        @pl.loop(0, span // block)
        def _(i):
            at = pl.ds(pl.multiple_of(b * span + i * block, block), block)
            step = adam_step(gdn[0:hidden_units, at], mdn[:, at], vdn[:, at])
            sdn[:, at] = jnp.where(leaves, 0.0, step).astype(BF16)
            leave_dn[at, :] = jnp.where(leaves, step, 0.0).T.astype(BF16)

    out_dn = pltpu.make_async_copy(sdn, sdn_hbm, out_sem.at[1])
    out_dn.start()
    sort_tiles(1, leave_dn)

    pass_on(1)

    for axis in range(2):
        for side in range(2):
            for late in range(2):
                ring_copy(axis, side, late).wait_recv()
        summed[axis] = tiles[axis, ring_at[axis]] + got[axis, 0] + got[axis, 1]
        for far in range(1, SIDE):
            fin_copy(axis, far).start()

    for axis in range(2):
        for far in range(1, SIDE):
            fin_copy(axis, far).wait_recv()
        mine = pl.ds(line_at[axis] * 2, 2)
        summed[axis, mine] = summed[axis, mine] + fin[axis, 0] + fin[axis, 1] + fin[axis, 2]
        last_copy(axis).start()

    for axis, adopted in ((0, aup_ref), (1, adn_ref)):
        last_copy(axis).wait_recv()
        adopted[...] = summed[axis, line_at[axis] * 2 + zhi] + last[axis]

    for axis in range(2):
        for side in range(2):
            hop_copy(axis, side).wait_send()
            for late in range(2):
                ring_copy(axis, side, late).wait_send()
        for far in range(1, SIDE):
            fin_copy(axis, far).wait_send()
        last_copy(axis).wait_send()

    @pl.loop(0, chunks)
    def _(chunk):
        @pl.loop(1, COLS)
        def _(i):
            plane_copy(chunk, i).wait_send()

        other_inner(chunk).wait_send()
        chain_full(z, chunk, 0).wait_send()

        @pl.when(edge)
        def _():
            transit_edge(chunk).wait_send()
            hand_thin(z, chunk).wait_send()

            @pl.loop(1, 3)
            def _(far):
                chain_full(toward_out(far), chunk, 0).wait_send()
                hand_thin(toward_out(far), chunk).wait_send()

            @pl.loop(1, 6)
            def _(far):
                hand_thin(toward_out(-far), chunk).wait_send()

        @pl.when(inner)
        def _():
            chain_thin(z, chunk, 1).wait_send()
            hand_full(z, chunk).wait_send()

            @pl.loop(1, 4)
            def _(far):
                chain_full(toward_out(far), chunk, 0).wait_send()
                hand_full(toward_out(far), chunk).wait_send()

            @pl.loop(1, 5)
            def _(far):
                chain_thin(toward_out(-far), chunk, 0).wait_send()
                hand_full(toward_out(-far), chunk).wait_send()

    @pl.when(edge)
    def _():
        for i in range(2):
            ward_weights(i).wait_send()

    @pl.when(inner)
    def _():
        @pl.loop(0, RING)
        def _(slot):
            pg_copy(slot).wait_send()

        @pl.loop(0, gd_out.shape[0])
        def _(b):
            gd_copy(b).wait_send()

    out_up.wait()
    out_dn.wait()


def expert_steps(leaving, adopt, routes, gates, tokens, cotangent, w_up, w_down, m_up, v_up, m_down, v_down):
    count, model_width = tokens.shape
    hidden = w_up.shape[1]
    chunks = model_width // 2 // WIDTH
    tile_rows = model_width // adopt.shape[0]
    smem = pl.BlockSpec(memory_space=pltpu.SMEM)
    vmem = pl.BlockSpec(memory_space=pltpu.VMEM)
    anyw = pl.BlockSpec(memory_space=pl.ANY)
    dma = pltpu.SemaphoreType.DMA
    return pl.pallas_call(
        kernel,
        out_shape=(
            jax.ShapeDtypeStruct((model_width, hidden), BF16),
            jax.ShapeDtypeStruct((hidden, model_width), BF16),
            jax.ShapeDtypeStruct((tile_rows, hidden), BF16),
            jax.ShapeDtypeStruct((tile_rows, hidden), BF16),
        ),
        in_specs=[vmem, smem, vmem, vmem] + [anyw] * 8,
        out_specs=(anyw, anyw, vmem, vmem),
        scratch_shapes=[
            pltpu.VMEM((count, model_width), BF16),
            pltpu.VMEM((count, model_width), BF16),
            pltpu.VMEM((model_width, hidden), BF16),
            pltpu.VMEM((hidden, model_width), BF16),
            pltpu.VMEM((model_width, hidden), BF16),
            pltpu.VMEM((hidden, model_width), BF16),
            pltpu.VMEM((model_width, hidden), BF16),
            pltpu.VMEM((model_width, hidden), BF16),
            pltpu.VMEM((hidden, model_width), BF16),
            pltpu.VMEM((hidden, model_width), BF16),
            pltpu.VMEM((model_width, hidden), BF16),
            pltpu.VMEM((hidden, model_width), BF16),
            pltpu.VMEM((ALL, PARTS * count), BF16),
            pltpu.VMEM((PARTS * 2 * UNIT, ALL), BF16),
            pltpu.VMEM((chunks, COLS, MSG, WIDTH), BF16),
            pltpu.VMEM((chunks, COLS, MSG, WIDTH), BF16),
            pltpu.VMEM((RING, 2, chunks, 2, UNIT, 2 * WIDTH), BF16),
            pltpu.VMEM((chunks, 2, UNIT, 2 * WIDTH), BF16),
            pltpu.VMEM((chunks, 2, UNIT, 2 * WIDTH), BF16),
            pltpu.VMEM((hidden, model_width), F32),
            pltpu.VMEM((2 * hidden, model_width), F32),
            pltpu.VMEM((RING, 2 * UNIT, hidden), BF16),
            pltpu.VMEM((RING, 2 * UNIT, hidden), BF16),
            pltpu.VMEM((7, hidden, model_width // 7), BF16),
            pltpu.VMEM((7, hidden, model_width // 7), BF16),
            pltpu.VMEM((model_width, hidden), BF16),
            pltpu.VMEM((model_width, hidden), BF16),
            pltpu.VMEM((2 * COLS, tile_rows, hidden), BF16),
            pltpu.VMEM((2, SIDE, 2 * SIDE, tile_rows, hidden), BF16),
            pltpu.VMEM((2, 2, SIDE, tile_rows, hidden), BF16),
            pltpu.VMEM((2, 2, 2 * SIDE, tile_rows, hidden), BF16),
            pltpu.VMEM((2, 2 * SIDE, tile_rows, hidden), BF16),
            pltpu.VMEM((2, SIDE - 1, 2, tile_rows, hidden), BF16),
            pltpu.VMEM((2, tile_rows, hidden), BF16),
            dma((8,)),
            dma((2,)),
            dma((chunks, COLS)),
            dma((chunks, COLS)),
            dma((chunks,)),
            dma((2, RING, chunks)),
            dma((RING, chunks)),
            dma((chunks,)),
            dma((chunks,)),
            dma((chunks,)),
            dma((RING, chunks)),
            dma((RING, chunks)),
            dma((2,)),
            dma((2,)),
            dma((RING,)),
            dma((RING,)),
            dma((7,)),
            dma((7,)),
            dma((2, 2)),
            dma((2, 2)),
            dma((2, 2, 2)),
            dma((2, 2, 2)),
            dma((2, SIDE - 1)),
            dma((2, SIDE - 1)),
            dma((2,)),
            dma((2,)),
        ],
        compiler_params=pltpu.CompilerParams(
            collective_id=0, has_side_effects=True, vmem_limit_bytes=62 * 1024 * 1024
        ),
        name="expert_steps",
    )(leaving, adopt, routes, gates, tokens, cotangent, w_up, w_down, m_up, v_up, m_down, v_down)


def on_device(
    tokens, cotangent, gates, routes, w_up, w_down, m_up, v_up, m_down, v_down, leaving, tile_owner
):
    experts = lax.axis_size("expert")
    tok_count = tokens.shape[0]
    slot_ids = jnp.arange(experts, dtype=jnp.int32)
    adopt = jnp.sum(
        jnp.where(tile_owner[None, :] == slot_ids[:, None], slot_ids[None, :], 0), axis=1
    )
    outs = expert_steps(
        leaving.reshape(1, 1),
        adopt,
        routes.reshape(1, tok_count),
        gates.reshape(1, tok_count),
        tokens,
        cotangent,
        w_up[0],
        w_down[0],
        m_up[0],
        v_up[0],
        m_down[0],
        v_down[0],
    )
    return tuple(out[None] for out in outs)


def solution(mesh):
    placed = (
        P(("dp", "expert"), None),
        P(("dp", "expert"), None),
        P(("dp", "expert"), None),
        P(("dp", "expert"), None),
        P("expert", None, "dp"),
        P("expert", "dp", None),
        P("expert", None, "dp"),
        P("expert", None, "dp"),
        P("expert", "dp", None),
        P("expert", "dp", None),
        P(),
        P(),
    )
    return jax.shard_map(
        on_device,
        mesh=mesh,
        in_specs=placed,
        out_specs=(
            P("expert", None, "dp"),
            P("expert", "dp", None),
            P("expert", None, "dp"),
            P("expert", None, "dp"),
        ),
        check_vma=False,
    )
```

```python
import functools

import jax
import jax.numpy as jnp
from jax import lax
from jax.experimental import pallas as pl
from jax.experimental.pallas import tpu as pltpu
from jax.sharding import PartitionSpec as P

BETA_ONE = 0.9
BETA_TWO = 0.95
EPSILON = 1e-08

MESH = pl.DeviceIdType.MESH
F32 = jnp.float32
BF16 = jnp.bfloat16

SLOTS = 5
COLS = 16
SIDE = 4
HALF = 4
RING = 8
PARTS = 4
WIDTH = 256
MSG = PARTS * 2 * SLOTS
UNIT = COLS * SLOTS
ALL = COLS * MSG
LAG = 2


def mul_t(a, b):
    return lax.dot_general(a, b, (((1,), (1,)), ((), ())), preferred_element_type=F32)


def mul(a, b):
    return lax.dot_general(a, b, (((1,), (0,)), ((), ())), preferred_element_type=F32)


def adam_step(gradient, moment_one, moment_two):
    new_one = BETA_ONE * moment_one.astype(F32) + (1.0 - BETA_ONE) * gradient
    new_two = BETA_TWO * moment_two.astype(F32) + (1.0 - BETA_TWO) * gradient * gradient
    return new_one / (jnp.sqrt(new_two) + EPSILON)


def kernel(
    leaving_ref, owner_ref, routes_ref, gates_ref, tok_hbm, cot_hbm, wup_hbm, wdn_hbm, mup_hbm, vup_hbm, mdn_hbm, vdn_hbm,
    sup_hbm, sdn_hbm, adopted_ref,
    tok, cot, wup, wdn, wup_ward, wdn_ward, mup, vup, mdn, vdn, sup, sdn,
    pick, unpick, packed, landed, own, other, transit, gup, gdn, pg_out, pg_in, gd_out, gd_in,
    adopt_ref, leave_up, leave_dn, by_tile, tiles, hop, got, summed, fin, last,
    load_sem, out_sem, plane_send, plane_recv, plane_self,
    chain_send, chain_recv, other_send, transit_send, transit_recv, mate_send, mate_recv,
    ward_send, ward_recv, pg_send, pg_recv, gd_send, gd_recv, hop_send, hop_recv, ring_send, ring_recv, fin_send, fin_recv, last_send, last_recv,
):
    chunks = packed.shape[0]
    half_width = tok.shape[1] // 2
    dp = lax.axis_index("dp")
    ex = lax.axis_index("expert")
    core = lax.rem(dp, 2)
    pos = dp // 2
    zhi = lax.rem(ex, 2)
    col = ex // 2
    cy, cx = col // SIDE, lax.rem(col, SIDE)
    z = zhi * HALF + pos
    me_other = 1 - zhi

    def at_z(z_to):
        return ((z_to % HALF) * 2 + core, col * 2 + z_to // HALF)

    znext, zprev = lax.rem(z + 1, RING), lax.rem(z + RING - 1, RING)
    mate = (pos * 2 + (1 - core), ex)

    def peer_col(i):
        return lax.rem(cy + i // SIDE, SIDE) * SIDE + lax.rem(cx + i % SIDE, SIDE)

    barrier = pltpu.get_barrier_semaphore()
    for i in range(1, COLS):
        pl.semaphore_signal(
            barrier, inc=1, device_id=(dp, peer_col(i) * 2 + zhi), device_id_type=MESH
        )
    twin = (dp, col * 2 + me_other)
    for who in (at_z(znext), at_z(zprev), mate, twin):
        pl.semaphore_signal(barrier, inc=1, device_id=who, device_id_type=MESH)

    loads = [
        pltpu.make_async_copy(src, dst, load_sem.at[i])
        for i, (src, dst) in enumerate(
            (
                (tok_hbm, tok),
                (cot_hbm, cot),
                (wup_hbm, wup),
                (wdn_hbm, wdn),
                (mup_hbm, mup),
                (vup_hbm, vup),
                (mdn_hbm, mdn),
                (vdn_hbm, vdn),
            )
        )
    ]
    for load in loads:
        load.start()

    count = tok.shape[0]
    routes = routes_ref[...]
    expert_ids = lax.broadcasted_iota(jnp.int32, (2 * COLS, count), 0)
    member = (expert_ids == routes).astype(F32)
    before = (
        lax.broadcasted_iota(jnp.int32, (count, count), 0)
        < lax.broadcasted_iota(jnp.int32, (count, count), 1)
    ).astype(BF16)
    rank = jnp.sum(member * mul(member.astype(BF16), before), axis=0, keepdims=True)
    place = (routes >> 1) * MSG + (routes & 1) * SLOTS + rank.astype(jnp.int32)
    eye = lax.broadcasted_iota(jnp.int32, (count, count), 0) == lax.broadcasted_iota(
        jnp.int32, (count, count), 1
    )
    gates = jnp.sum(
        jnp.where(eye, jnp.broadcast_to(gates_ref[...], (count, count)), 0.0), axis=1, keepdims=True
    )
    target = lax.broadcasted_iota(jnp.int32, (ALL, count), 0)
    for part in range(PARTS):
        pick[:, part * count : (part + 1) * count] = (target == place + part * 2 * SLOTS).astype(
            F32
        ).astype(BF16)

    pl.semaphore_wait(barrier, COLS - 1 + 4)

    upper = pos >= 2
    edge = (pos == 0) | (pos == HALF - 1)
    inner = jnp.logical_not(edge)
    out_sign = jnp.where(upper, 1, -1)
    z_out = lax.rem(z + RING + out_sign, RING)
    z_in = lax.rem(z + RING - out_sign, RING)

    def ward_weights(i):
        src, dst = ((wup, wup_ward), (wdn, wdn_ward))[i]
        return pltpu.make_async_remote_copy(
            src_ref=src,
            dst_ref=dst,
            send_sem=ward_send.at[i],
            recv_sem=ward_recv.at[i],
            device_id=at_z(z_in),
            device_id_type=MESH,
        )

    for load in loads[:4]:
        load.wait()

    @pl.when(edge)
    def _():
        for i in range(2):
            ward_weights(i).start()


    def lanes(chunk, high):
        return pl.ds(pl.multiple_of(high * half_width + chunk * WIDTH, 128), WIDTH)

    def plane_copy(chunk, i):
        to = peer_col(i)
        return pltpu.make_async_remote_copy(
            src_ref=packed.at[chunk, to],
            dst_ref=landed.at[chunk, col],
            send_sem=plane_send.at[chunk, i],
            recv_sem=plane_recv.at[chunk, i],
            device_id=(dp, to * 2 + zhi),
            device_id_type=MESH,
        )

    def plane_keep(chunk):
        return pltpu.make_async_copy(
            packed.at[chunk, col], landed.at[chunk, col], plane_self.at[chunk]
        )

    @pl.loop(0, chunks)
    def _(chunk):
        both = [tok[:, lanes(chunk, h)] for h in range(2)]
        both += [
            (gates * cot[:, lanes(chunk, h)].astype(F32)).astype(BF16) for h in range(2)
        ]
        rows = mul(pick[...], jnp.concatenate(both, axis=0))
        packed[chunk] = rows.reshape(COLS, MSG, WIDTH).astype(BF16)
        plane_keep(chunk).start()

        @pl.loop(1, COLS)
        def _(i):
            plane_copy(chunk, i).start()

    @pl.loop(0, 2 * COLS)
    def _(owner):
        mine = jnp.int32(0)
        for tile in range(2 * COLS):
            mine = jnp.where(owner_ref[tile] == owner, jnp.int32(tile), mine)
        adopt_ref[owner] = mine

    line = lax.broadcasted_iota(jnp.int32, (UNIT, ALL), 0)
    source = lax.broadcasted_iota(jnp.int32, (UNIT, ALL), 1)
    fifth = (line * 205) >> 10
    base = fifth * MSG + (line - fifth * SLOTS)
    for part in range(PARTS):
        for which, half in ((0, zhi), (1, me_other)):
            start = (part * 2 + which) * UNIT
            unpick[start : start + UNIT, :] = (
                (source == base + (part * 2 * SLOTS + half * SLOTS)).astype(F32).astype(BF16)
            )

    gup[...] = jnp.zeros_like(gup)
    gdn[...] = jnp.zeros_like(gdn)

    def chain_full(slot, chunk, sem):
        return pltpu.make_async_remote_copy(
            src_ref=own.at[slot, core, chunk],
            dst_ref=own.at[slot, core, chunk],
            send_sem=chain_send.at[sem, slot, chunk],
            recv_sem=chain_recv.at[slot, chunk],
            device_id=at_z(z_in),
            device_id_type=MESH,
        )

    def chain_thin(slot, chunk, sem):
        return pltpu.make_async_remote_copy(
            src_ref=own.at[slot, core, chunk, 0],
            dst_ref=own.at[slot, core, chunk, 0],
            send_sem=chain_send.at[sem, slot, chunk],
            recv_sem=chain_recv.at[slot, chunk],
            device_id=at_z(z_out),
            device_id_type=MESH,
        )

    def hand_full(slot, chunk):
        return pltpu.make_async_remote_copy(
            src_ref=own.at[slot, core, chunk],
            dst_ref=own.at[slot, core, chunk],
            send_sem=mate_send.at[slot, chunk],
            recv_sem=mate_recv.at[slot, chunk],
            device_id=mate,
            device_id_type=MESH,
        )

    def hand_thin(slot, chunk):
        return pltpu.make_async_remote_copy(
            src_ref=own.at[slot, core, chunk, 0],
            dst_ref=own.at[slot, core, chunk, 0],
            send_sem=mate_send.at[slot, chunk],
            recv_sem=mate_recv.at[slot, chunk],
            device_id=mate,
            device_id_type=MESH,
        )

    def other_inner(chunk):
        return pltpu.make_async_remote_copy(
            src_ref=other.at[chunk],
            dst_ref=transit.at[chunk],
            send_sem=other_send.at[chunk],
            recv_sem=transit_recv.at[chunk],
            device_id=at_z(z_out),
            device_id_type=MESH,
        )

    def other_edge(chunk):
        return pltpu.make_async_remote_copy(
            src_ref=other.at[chunk],
            dst_ref=own.at[z, core, chunk],
            send_sem=other_send.at[chunk],
            recv_sem=chain_recv.at[z, chunk],
            device_id=at_z(z_out),
            device_id_type=MESH,
        )

    def transit_edge(chunk):
        return pltpu.make_async_remote_copy(
            src_ref=transit.at[chunk],
            dst_ref=own.at[z_in, core, chunk],
            send_sem=transit_send.at[chunk],
            recv_sem=chain_recv.at[z_in, chunk],
            device_id=at_z(z_out),
            device_id_type=MESH,
        )

    def pg_copy(slot):
        return pltpu.make_async_remote_copy(
            src_ref=pg_out.at[slot],
            dst_ref=pg_in.at[slot],
            send_sem=pg_send.at[slot],
            recv_sem=pg_recv.at[slot],
            device_id=at_z(z_out),
            device_id_type=MESH,
        )

    def gd_copy(b):
        return pltpu.make_async_remote_copy(
            src_ref=gd_out.at[b],
            dst_ref=gd_in.at[b],
            send_sem=gd_send.at[b],
            recv_sem=gd_recv.at[b],
            device_id=at_z(z_out),
            device_id_type=MESH,
        )

    @pl.loop(0, chunks)
    def _(chunk):
        plane_keep(chunk).wait()

        @pl.loop(1, COLS)
        def _(i):
            plane_copy(chunk, i).wait_recv()

        rows = mul(
            unpick[...], landed[chunk].astype(F32).reshape(ALL, WIDTH).astype(BF16)
        ).astype(BF16)
        for part in range(PARTS):
            start = part * 2 * UNIT
            kind, high = part // 2, part % 2
            at = slice(high * WIDTH, (high + 1) * WIDTH)
            own[z, core, chunk, kind, :, at] = rows[start : start + UNIT]
            other[chunk, kind, :, at] = rows[start + UNIT : start + 2 * UNIT]

        @pl.when(edge)
        def _():
            other_edge(chunk).start()
            chain_full(z, chunk, 0).start()
            hand_thin(z, chunk).start()

        @pl.when(inner)
        def _():
            other_inner(chunk).start()
            chain_full(z, chunk, 0).start()
            chain_thin(z, chunk, 1).start()
            hand_full(z, chunk).start()

    for load in loads[4:]:
        load.wait()

    hidden_units = wup.shape[1]

    def pair(slot, chunk, kind, high):
        at = slice(high * WIDTH, (high + 1) * WIDTH)
        return jnp.concatenate(
            [own[slot, 0, chunk, kind, :, at], own[slot, 1, chunk, kind, :, at]], axis=0
        )

    def places():
        for chunk in range(chunks):
            for high in range(2):
                yield chunk, high, high * half_width + chunk * WIDTH

    def terms_inner(slot):
        @pl.loop(0, chunks)
        def _(chunk):
            hand_full(slot, chunk).wait_recv()

        preact = jnp.zeros((2 * UNIT, 2 * hidden_units), F32)
        back = jnp.zeros((2 * UNIT, 2 * hidden_units), F32)
        for chunk, high, at in places():
            here = slice(at, at + WIDTH)
            preact += mul(
                pair(slot, chunk, 0, high),
                jnp.concatenate([wup[here, :], wup_ward[here, :]], axis=1),
            )
            back += mul_t(
                pair(slot, chunk, 1, high),
                jnp.concatenate([wdn[:, here], wdn_ward[:, here]], axis=0),
            )
        squash = jax.nn.sigmoid(preact)
        hidden = preact * squash
        pre_grad = (back * (squash * (1.0 + preact * (1.0 - squash)))).astype(BF16)
        pg_out[slot] = pre_grad[:, hidden_units:]
        hidden = hidden.astype(BF16).astype(F32).T.astype(BF16)
        pre_grad = pre_grad[:, :hidden_units].astype(F32).T.astype(BF16)
        pg_copy(slot).start()
        for chunk, high, at in places():
            here = slice(at, at + WIDTH)
            gdn[:, here] += mul(hidden, pair(slot, chunk, 1, high))
            gup[:, here] += mul(pre_grad, pair(slot, chunk, 0, high))

    def terms_edge(slot):
        @pl.loop(0, chunks)
        def _(chunk):
            hand_thin(slot, chunk).wait_recv()

        pg_copy(slot).wait_recv()
        pre_grad = pg_in[slot].astype(F32).T.astype(BF16)
        for chunk, high, at in places():
            gup[:, at : at + WIDTH] += mul(pre_grad, pair(slot, chunk, 0, high))

    def toward_out(far):
        return lax.rem(z + RING + out_sign * far, RING)

    def relay_out(far, chunk):
        slot = toward_out(far)
        chain_full(slot, chunk, 0).wait_recv()
        chain_full(slot, chunk, 0).start()

        @pl.when(edge)
        def _():
            hand_thin(slot, chunk).start()

        @pl.when(inner)
        def _():
            hand_full(slot, chunk).start()

    def relay_in(far, chunk):
        slot = toward_out(-far)
        chain_full(slot, chunk, 0).wait_recv()
        chain_thin(slot, chunk, 0).start()
        hand_full(slot, chunk).start()

    def edge_unit(i):
        thin = (i == 0) | (lax.rem(i, 2) == 1)
        far = jnp.where(i == 0, 1, (i + 3) // 2)
        return thin, toward_out(jnp.where(thin, -far, i // 2 - 1))

    @pl.when(edge)
    def _():
        @pl.loop(0, chunks)
        def _(chunk):
            other_inner(chunk).wait_recv()
            transit_edge(chunk).start()
            relay_out(1, chunk)

        @pl.loop(0, chunks)
        def _(chunk):
            relay_out(2, chunk)

        @pl.loop(0, RING)
        def _(i):
            thin, slot = edge_unit(i)

            @pl.when(thin)
            def _():
                @pl.loop(0, chunks)
                def _(chunk):
                    chain_thin(slot, chunk, 0).wait_recv()
                    hand_thin(slot, chunk).start()

            terms_edge(slot)

    @pl.when(inner)
    def _():
        @pl.loop(0, chunks)
        def _(chunk):
            relay_in(1, chunk)

        for i in range(2):
            ward_weights(i).wait_recv()

        def relay_in_at(item):
            relay_in(item // chunks + 1, lax.rem(item, chunks))

        steps = (HALF - 1) * chunks

        @pl.loop(0, steps)
        def _(item):
            relay_out(item // chunks + 1, lax.rem(item, chunks))

            @pl.when(item >= LAG)
            def _():
                relay_in_at(item + chunks - LAG)

            @pl.when(lax.rem(item, 3) == 2)
            def _():
                turn = item // 3
                terms_inner(
                    toward_out(jnp.where(lax.rem(turn, 2) == 0, turn // 2, -((turn + 1) // 2)))
                )

        @pl.loop(0, LAG)
        def _(i):
            relay_in_at(steps + chunks - LAG + i)

        terms_inner(toward_out(-HALF))

        span = gd_out.shape[2]
        for b in range(gd_out.shape[0]):
            gd_out[b] = gdn[hidden_units:, b * span : (b + 1) * span].astype(BF16)
            gd_copy(b).start()

    model_width = tok.shape[1]
    block = 128
    leaves = jnp.broadcast_to(leaving_ref[...], (block, block)) == ex
    ring_at, line_at = (cx, cy), (cy, cx)
    middle = SIDE

    def tile_home(axis, ring_to, line_to):
        to = line_to * SIDE + ring_to if axis == 0 else ring_to * SIDE + line_to
        return (dp, to * 2 + zhi)

    def ring_next(axis, far):
        return lax.rem(ring_at[axis] + far, SIDE)

    def ring_to(axis, side):
        return tile_home(axis, ring_next(axis, 1 if side == 0 else SIDE - 1), line_at[axis])

    def part_of(side):
        return pl.ds(0, middle) if side == 0 else pl.ds(middle, middle)

    def hop_copy(axis, side):
        return pltpu.make_async_remote_copy(
            src_ref=tiles.at[axis, ring_next(axis, 2), part_of(side)],
            dst_ref=hop.at[axis, side],
            send_sem=hop_send.at[axis, side],
            recv_sem=hop_recv.at[axis, side],
            device_id=ring_to(axis, side),
            device_id_type=MESH,
        )

    def ring_copy(axis, side, late):
        part = part_of(side if late else 1 - side)
        return pltpu.make_async_remote_copy(
            src_ref=tiles.at[axis, ring_next(axis, 1 if side == 0 else SIDE - 1), part],
            dst_ref=got.at[axis, side, part],
            send_sem=ring_send.at[axis, side, late],
            recv_sem=ring_recv.at[axis, side, late],
            device_id=ring_to(axis, side),
            device_id_type=MESH,
        )

    def fin_copy(axis, far):
        line_to = lax.rem(line_at[axis] + far, SIDE)
        return pltpu.make_async_remote_copy(
            src_ref=summed.at[axis, pl.ds(line_to * 2, 2)],
            dst_ref=fin.at[axis, far - 1],
            send_sem=fin_send.at[axis, far - 1],
            recv_sem=fin_recv.at[axis, far - 1],
            device_id=tile_home(axis, ring_at[axis], line_to),
            device_id_type=MESH,
        )

    def last_copy(axis):
        return pltpu.make_async_remote_copy(
            src_ref=summed.at[axis, line_at[axis] * 2 + me_other],
            dst_ref=last.at[axis],
            send_sem=last_send.at[axis],
            recv_sem=last_recv.at[axis],
            device_id=twin,
            device_id_type=MESH,
        )

    def sort_tiles(axis, leave):
        rows = tiles.shape[3]
        for tile in range(2 * COLS):
            by_tile[tile] = leave[tile * rows : (tile + 1) * rows, :]

        @pl.loop(0, 2 * COLS)
        def _(owner):
            to = owner // 2
            ty, tx = to // SIDE, lax.rem(to, SIDE)
            r, l = (tx, ty) if axis == 0 else (ty, tx)
            tiles[axis, r, l * 2 + lax.rem(owner, 2)] = by_tile[adopt_ref[owner]]

        for side in range(2):
            hop_copy(axis, side).start()
        for side in range(2):
            ring_copy(axis, side, 0).start()

    @pl.loop(0, model_width // block)
    def _(b):
        at = pl.ds(pl.multiple_of(b * block, block), block)
        step = adam_step(gup[:, at].T, mup[at, :], vup[at, :])
        sup[at, :] = step.astype(BF16)
        leave_up[at, :] = jnp.where(leaves, step, 0.0).astype(BF16)

    out_up = pltpu.make_async_copy(sup, sup_hbm, out_sem.at[0])
    out_up.start()
    sort_tiles(0, leave_up)

    def pass_on(axis):
        for side in range(2):
            hop_copy(axis, side).wait_recv()
            to = ring_next(axis, 1 if side == 0 else SIDE - 1)
            part = part_of(side)
            tiles[axis, to, part] = tiles[axis, to, part] + hop[axis, side]
            ring_copy(axis, side, 1).start()

    pass_on(0)
    span = gd_in.shape[2]

    @pl.loop(0, gd_in.shape[0])
    def _(b):
        @pl.when(edge)
        def _():
            gd_copy(b).wait_recv()
            gdn[0:hidden_units, pl.ds(pl.multiple_of(b * span, block), span)] = gd_in[b].astype(F32)

        @pl.loop(0, span // block)
        def _(i):
            at = pl.ds(pl.multiple_of(b * span + i * block, block), block)
            step = adam_step(gdn[0:hidden_units, at], mdn[:, at], vdn[:, at])
            sdn[:, at] = step.astype(BF16)
            leave_dn[at, :] = jnp.where(leaves, step, 0.0).T.astype(BF16)

    out_dn = pltpu.make_async_copy(sdn, sdn_hbm, out_sem.at[1])
    out_dn.start()
    sort_tiles(1, leave_dn)

    pass_on(1)

    for axis in range(2):
        for side in range(2):
            for late in range(2):
                ring_copy(axis, side, late).wait_recv()
        summed[axis] = tiles[axis, ring_at[axis]] + got[axis, 0] + got[axis, 1]
        for far in range(1, SIDE):
            fin_copy(axis, far).start()

    for axis in range(2):
        for far in range(1, SIDE):
            fin_copy(axis, far).wait_recv()
        mine = pl.ds(line_at[axis] * 2, 2)
        summed[axis, mine] = summed[axis, mine] + fin[axis, 0] + fin[axis, 1] + fin[axis, 2]
        last_copy(axis).start()

    for axis in range(2):
        last_copy(axis).wait_recv()
        adopted_ref[axis] = summed[axis, line_at[axis] * 2 + zhi] + last[axis]

    for axis in range(2):
        for side in range(2):
            hop_copy(axis, side).wait_send()
            for late in range(2):
                ring_copy(axis, side, late).wait_send()
        for far in range(1, SIDE):
            fin_copy(axis, far).wait_send()
        last_copy(axis).wait_send()

    @pl.loop(0, chunks)
    def _(chunk):
        @pl.loop(1, COLS)
        def _(i):
            plane_copy(chunk, i).wait_send()

        other_inner(chunk).wait_send()
        chain_full(z, chunk, 0).wait_send()

        @pl.when(edge)
        def _():
            transit_edge(chunk).wait_send()
            hand_thin(z, chunk).wait_send()

            @pl.loop(1, 3)
            def _(far):
                chain_full(toward_out(far), chunk, 0).wait_send()
                hand_thin(toward_out(far), chunk).wait_send()

            @pl.loop(1, 6)
            def _(far):
                hand_thin(toward_out(-far), chunk).wait_send()

        @pl.when(inner)
        def _():
            chain_thin(z, chunk, 1).wait_send()
            hand_full(z, chunk).wait_send()

            @pl.loop(1, 4)
            def _(far):
                chain_full(toward_out(far), chunk, 0).wait_send()
                hand_full(toward_out(far), chunk).wait_send()

            @pl.loop(1, 5)
            def _(far):
                chain_thin(toward_out(-far), chunk, 0).wait_send()
                hand_full(toward_out(-far), chunk).wait_send()

    @pl.when(edge)
    def _():
        for i in range(2):
            ward_weights(i).wait_send()

    @pl.when(inner)
    def _():
        @pl.loop(0, RING)
        def _(slot):
            pg_copy(slot).wait_send()

        @pl.loop(0, gd_out.shape[0])
        def _(b):
            gd_copy(b).wait_send()

    out_up.wait()
    out_dn.wait()


def expert_steps(leaving, tile_owner, routes, gates, tokens, cotangent, w_up, w_down, m_up, v_up, m_down, v_down):
    count, model_width = tokens.shape
    hidden = w_up.shape[1]
    chunks = model_width // 2 // WIDTH
    tile_rows = model_width // tile_owner.shape[0]
    smem = pl.BlockSpec(memory_space=pltpu.SMEM)
    vmem = pl.BlockSpec(memory_space=pltpu.VMEM)
    anyw = pl.BlockSpec(memory_space=pl.ANY)
    dma = pltpu.SemaphoreType.DMA
    return pl.pallas_call(
        kernel,
        out_shape=(
            jax.ShapeDtypeStruct((model_width, hidden), BF16),
            jax.ShapeDtypeStruct((hidden, model_width), BF16),
            jax.ShapeDtypeStruct((2, tile_rows, hidden), BF16),
        ),
        in_specs=[vmem, smem, vmem, vmem] + [anyw] * 8,
        out_specs=(anyw, anyw, vmem),
        scratch_shapes=[
            pltpu.VMEM((count, model_width), BF16),
            pltpu.VMEM((count, model_width), BF16),
            pltpu.VMEM((model_width, hidden), BF16),
            pltpu.VMEM((hidden, model_width), BF16),
            pltpu.VMEM((model_width, hidden), BF16),
            pltpu.VMEM((hidden, model_width), BF16),
            pltpu.VMEM((model_width, hidden), BF16),
            pltpu.VMEM((model_width, hidden), BF16),
            pltpu.VMEM((hidden, model_width), BF16),
            pltpu.VMEM((hidden, model_width), BF16),
            pltpu.VMEM((model_width, hidden), BF16),
            pltpu.VMEM((hidden, model_width), BF16),
            pltpu.VMEM((ALL, PARTS * count), BF16),
            pltpu.VMEM((PARTS * 2 * UNIT, ALL), BF16),
            pltpu.VMEM((chunks, COLS, MSG, WIDTH), BF16),
            pltpu.VMEM((chunks, COLS, MSG, WIDTH), BF16),
            pltpu.VMEM((RING, 2, chunks, 2, UNIT, 2 * WIDTH), BF16),
            pltpu.VMEM((chunks, 2, UNIT, 2 * WIDTH), BF16),
            pltpu.VMEM((chunks, 2, UNIT, 2 * WIDTH), BF16),
            pltpu.VMEM((hidden, model_width), F32),
            pltpu.VMEM((2 * hidden, model_width), F32),
            pltpu.VMEM((RING, 2 * UNIT, hidden), BF16),
            pltpu.VMEM((RING, 2 * UNIT, hidden), BF16),
            pltpu.VMEM((7, hidden, model_width // 7), BF16),
            pltpu.VMEM((7, hidden, model_width // 7), BF16),
            pltpu.SMEM((2 * COLS,), jnp.int32),
            pltpu.VMEM((model_width, hidden), BF16),
            pltpu.VMEM((model_width, hidden), BF16),
            pltpu.VMEM((2 * COLS, tile_rows, hidden), BF16),
            pltpu.VMEM((2, SIDE, 2 * SIDE, tile_rows, hidden), BF16),
            pltpu.VMEM((2, 2, SIDE, tile_rows, hidden), BF16),
            pltpu.VMEM((2, 2, 2 * SIDE, tile_rows, hidden), BF16),
            pltpu.VMEM((2, 2 * SIDE, tile_rows, hidden), BF16),
            pltpu.VMEM((2, SIDE - 1, 2, tile_rows, hidden), BF16),
            pltpu.VMEM((2, tile_rows, hidden), BF16),
            dma((8,)),
            dma((2,)),
            dma((chunks, COLS)),
            dma((chunks, COLS)),
            dma((chunks,)),
            dma((2, RING, chunks)),
            dma((RING, chunks)),
            dma((chunks,)),
            dma((chunks,)),
            dma((chunks,)),
            dma((RING, chunks)),
            dma((RING, chunks)),
            dma((2,)),
            dma((2,)),
            dma((RING,)),
            dma((RING,)),
            dma((7,)),
            dma((7,)),
            dma((2, 2)),
            dma((2, 2)),
            dma((2, 2, 2)),
            dma((2, 2, 2)),
            dma((2, SIDE - 1)),
            dma((2, SIDE - 1)),
            dma((2,)),
            dma((2,)),
        ],
        compiler_params=pltpu.CompilerParams(
            collective_id=0, has_side_effects=True, vmem_limit_bytes=52 * 1024 * 1024
        ),
        name="expert_steps",
    )(leaving, tile_owner, routes, gates, tokens, cotangent, w_up, w_down, m_up, v_up, m_down, v_down)


def on_device(
    tokens, cotangent, gates, routes, w_up, w_down, m_up, v_up, m_down, v_down, leaving, tile_owner
):
    tok_count = tokens.shape[0]
    step_up, step_down, adopted = expert_steps(
        leaving.reshape(1, 1),
        tile_owner,
        routes.reshape(1, tok_count),
        gates.reshape(1, tok_count),
        tokens,
        cotangent,
        w_up[0],
        w_down[0],
        m_up[0],
        v_up[0],
        m_down[0],
        v_down[0],
    )
    keep_own = lax.axis_index("expert") != leaving[0]
    update_up = jnp.where(keep_own, step_up, jnp.zeros_like(step_up))[None]
    update_down = jnp.where(keep_own, step_down, jnp.zeros_like(step_down))[None]
    return (update_up, update_down, adopted[0][None], adopted[1][None])


def solution(mesh):
    placed = (
        P(("dp", "expert"), None),
        P(("dp", "expert"), None),
        P(("dp", "expert"), None),
        P(("dp", "expert"), None),
        P("expert", None, "dp"),
        P("expert", "dp", None),
        P("expert", None, "dp"),
        P("expert", None, "dp"),
        P("expert", "dp", None),
        P("expert", "dp", None),
        P(),
        P(),
    )
    return jax.shard_map(
        on_device,
        mesh=mesh,
        in_specs=placed,
        out_specs=(
            P("expert", None, "dp"),
            P("expert", "dp", None),
            P("expert", None, "dp"),
            P("expert", None, "dp"),
        ),
        check_vma=False,
    )
```

```python
import functools

import jax
import jax.numpy as jnp
from jax import lax
from jax.experimental import pallas as pl
from jax.experimental.pallas import tpu as pltpu
from jax.sharding import PartitionSpec as P

BETA_ONE = 0.9
BETA_TWO = 0.95
EPSILON = 1e-08

MESH = pl.DeviceIdType.MESH
F32 = jnp.float32
BF16 = jnp.bfloat16

SLOTS = 5
COLS = 16
SIDE = 4
HALF = 4
RING = 8
PARTS = 4
WIDTH = 256
MSG = PARTS * 2 * SLOTS
UNIT = COLS * SLOTS
ALL = COLS * MSG
LAG = 2


def mul_t(a, b):
    return lax.dot_general(a, b, (((1,), (1,)), ((), ())), preferred_element_type=F32)


def mul(a, b):
    return lax.dot_general(a, b, (((1,), (0,)), ((), ())), preferred_element_type=F32)


def adam_step(gradient, moment_one, moment_two):
    new_one = BETA_ONE * moment_one.astype(F32) + (1.0 - BETA_ONE) * gradient
    new_two = BETA_TWO * moment_two.astype(F32) + (1.0 - BETA_TWO) * gradient * gradient
    return new_one / (jnp.sqrt(new_two) + EPSILON)


def kernel(
    leaving_ref, owner_ref, routes_ref, gates_ref, tok_hbm, cot_hbm, wup_hbm, wdn_hbm, mup_hbm, vup_hbm, mdn_hbm, vdn_hbm,
    sup, sdn, adopted_ref,
    tok, cot, wup, wdn, wup_ward, wdn_ward, mup, vup, mdn, vdn,
    pick, unpick, packed, landed, own, other, transit, gup, gdn, pg_out, pg_in, gd_out, gd_in,
    adopt_ref, leave_up, leave_dn, by_tile, tiles, hop, got, summed, fin, last,
    load_sem, plane_send, plane_recv, plane_self,
    chain_send, chain_recv, other_send, transit_send, transit_recv, mate_send, mate_recv,
    ward_send, ward_recv, pg_send, pg_recv, gd_send, gd_recv, hop_send, hop_recv, ring_send, ring_recv, fin_send, fin_recv, last_send, last_recv,
):
    chunks = packed.shape[0]
    half_width = tok.shape[1] // 2
    dp = lax.axis_index("dp")
    ex = lax.axis_index("expert")
    core = lax.rem(dp, 2)
    pos = dp // 2
    zhi = lax.rem(ex, 2)
    col = ex // 2
    cy, cx = col // SIDE, lax.rem(col, SIDE)
    z = zhi * HALF + pos
    me_other = 1 - zhi

    def at_z(z_to):
        return ((z_to % HALF) * 2 + core, col * 2 + z_to // HALF)

    znext, zprev = lax.rem(z + 1, RING), lax.rem(z + RING - 1, RING)
    mate = (pos * 2 + (1 - core), ex)

    def peer_col(i):
        return lax.rem(cy + i // SIDE, SIDE) * SIDE + lax.rem(cx + i % SIDE, SIDE)

    barrier = pltpu.get_barrier_semaphore()
    for i in range(1, COLS):
        pl.semaphore_signal(
            barrier, inc=1, device_id=(dp, peer_col(i) * 2 + zhi), device_id_type=MESH
        )
    twin = (dp, col * 2 + me_other)
    for who in (at_z(znext), at_z(zprev), mate, twin):
        pl.semaphore_signal(barrier, inc=1, device_id=who, device_id_type=MESH)

    loads = [
        pltpu.make_async_copy(src, dst, load_sem.at[i])
        for i, (src, dst) in enumerate(
            (
                (tok_hbm, tok),
                (cot_hbm, cot),
                (wup_hbm, wup),
                (wdn_hbm, wdn),
                (mup_hbm, mup),
                (vup_hbm, vup),
                (mdn_hbm, mdn),
                (vdn_hbm, vdn),
            )
        )
    ]
    for load in loads:
        load.start()

    count = tok.shape[0]
    routes = routes_ref[...]
    expert_ids = lax.broadcasted_iota(jnp.int32, (2 * COLS, count), 0)
    member = (expert_ids == routes).astype(F32)
    before = (
        lax.broadcasted_iota(jnp.int32, (count, count), 0)
        < lax.broadcasted_iota(jnp.int32, (count, count), 1)
    ).astype(BF16)
    rank = jnp.sum(member * mul(member.astype(BF16), before), axis=0, keepdims=True)
    place = (routes >> 1) * MSG + (routes & 1) * SLOTS + rank.astype(jnp.int32)
    eye = lax.broadcasted_iota(jnp.int32, (count, count), 0) == lax.broadcasted_iota(
        jnp.int32, (count, count), 1
    )
    gates = jnp.sum(
        jnp.where(eye, jnp.broadcast_to(gates_ref[...], (count, count)), 0.0), axis=1, keepdims=True
    )
    target = lax.broadcasted_iota(jnp.int32, (ALL, count), 0)
    for part in range(PARTS):
        pick[:, part * count : (part + 1) * count] = (target == place + part * 2 * SLOTS).astype(
            F32
        ).astype(BF16)

    pl.semaphore_wait(barrier, COLS - 1 + 4)

    upper = pos >= 2
    edge = (pos == 0) | (pos == HALF - 1)
    inner = jnp.logical_not(edge)
    out_sign = jnp.where(upper, 1, -1)
    z_out = lax.rem(z + RING + out_sign, RING)
    z_in = lax.rem(z + RING - out_sign, RING)

    def ward_weights(i):
        src, dst = ((wup, wup_ward), (wdn, wdn_ward))[i]
        return pltpu.make_async_remote_copy(
            src_ref=src,
            dst_ref=dst,
            send_sem=ward_send.at[i],
            recv_sem=ward_recv.at[i],
            device_id=at_z(z_in),
            device_id_type=MESH,
        )

    for load in loads[:4]:
        load.wait()

    @pl.when(edge)
    def _():
        for i in range(2):
            ward_weights(i).start()


    def lanes(chunk, high):
        return pl.ds(pl.multiple_of(high * half_width + chunk * WIDTH, 128), WIDTH)

    def plane_copy(chunk, i):
        to = peer_col(i)
        return pltpu.make_async_remote_copy(
            src_ref=packed.at[chunk, to],
            dst_ref=landed.at[chunk, col],
            send_sem=plane_send.at[chunk, i],
            recv_sem=plane_recv.at[chunk, i],
            device_id=(dp, to * 2 + zhi),
            device_id_type=MESH,
        )

    def plane_keep(chunk):
        return pltpu.make_async_copy(
            packed.at[chunk, col], landed.at[chunk, col], plane_self.at[chunk]
        )

    @pl.loop(0, chunks)
    def _(chunk):
        both = [tok[:, lanes(chunk, h)] for h in range(2)]
        both += [
            (gates * cot[:, lanes(chunk, h)].astype(F32)).astype(BF16) for h in range(2)
        ]
        rows = mul(pick[...], jnp.concatenate(both, axis=0))
        packed[chunk] = rows.reshape(COLS, MSG, WIDTH).astype(BF16)
        plane_keep(chunk).start()

        @pl.loop(1, COLS)
        def _(i):
            plane_copy(chunk, i).start()

    @pl.loop(0, 2 * COLS)
    def _(owner):
        mine = jnp.int32(0)
        for tile in range(2 * COLS):
            mine = jnp.where(owner_ref[tile] == owner, jnp.int32(tile), mine)
        adopt_ref[owner] = mine

    line = lax.broadcasted_iota(jnp.int32, (UNIT, ALL), 0)
    source = lax.broadcasted_iota(jnp.int32, (UNIT, ALL), 1)
    fifth = (line * 205) >> 10
    base = fifth * MSG + (line - fifth * SLOTS)
    for part in range(PARTS):
        for which, half in ((0, zhi), (1, me_other)):
            start = (part * 2 + which) * UNIT
            unpick[start : start + UNIT, :] = (
                (source == base + (part * 2 * SLOTS + half * SLOTS)).astype(F32).astype(BF16)
            )

    gup[...] = jnp.zeros_like(gup)
    gdn[...] = jnp.zeros_like(gdn)

    def chain_full(slot, chunk, sem):
        return pltpu.make_async_remote_copy(
            src_ref=own.at[slot, core, chunk],
            dst_ref=own.at[slot, core, chunk],
            send_sem=chain_send.at[sem, slot, chunk],
            recv_sem=chain_recv.at[slot, chunk],
            device_id=at_z(z_in),
            device_id_type=MESH,
        )

    def chain_thin(slot, chunk, sem):
        return pltpu.make_async_remote_copy(
            src_ref=own.at[slot, core, chunk, 0],
            dst_ref=own.at[slot, core, chunk, 0],
            send_sem=chain_send.at[sem, slot, chunk],
            recv_sem=chain_recv.at[slot, chunk],
            device_id=at_z(z_out),
            device_id_type=MESH,
        )

    def hand_full(slot, chunk):
        return pltpu.make_async_remote_copy(
            src_ref=own.at[slot, core, chunk],
            dst_ref=own.at[slot, core, chunk],
            send_sem=mate_send.at[slot, chunk],
            recv_sem=mate_recv.at[slot, chunk],
            device_id=mate,
            device_id_type=MESH,
        )

    def hand_thin(slot, chunk):
        return pltpu.make_async_remote_copy(
            src_ref=own.at[slot, core, chunk, 0],
            dst_ref=own.at[slot, core, chunk, 0],
            send_sem=mate_send.at[slot, chunk],
            recv_sem=mate_recv.at[slot, chunk],
            device_id=mate,
            device_id_type=MESH,
        )

    def other_inner(chunk):
        return pltpu.make_async_remote_copy(
            src_ref=other.at[chunk],
            dst_ref=transit.at[chunk],
            send_sem=other_send.at[chunk],
            recv_sem=transit_recv.at[chunk],
            device_id=at_z(z_out),
            device_id_type=MESH,
        )

    def other_edge(chunk):
        return pltpu.make_async_remote_copy(
            src_ref=other.at[chunk],
            dst_ref=own.at[z, core, chunk],
            send_sem=other_send.at[chunk],
            recv_sem=chain_recv.at[z, chunk],
            device_id=at_z(z_out),
            device_id_type=MESH,
        )

    def transit_edge(chunk):
        return pltpu.make_async_remote_copy(
            src_ref=transit.at[chunk],
            dst_ref=own.at[z_in, core, chunk],
            send_sem=transit_send.at[chunk],
            recv_sem=chain_recv.at[z_in, chunk],
            device_id=at_z(z_out),
            device_id_type=MESH,
        )

    def pg_copy(slot):
        return pltpu.make_async_remote_copy(
            src_ref=pg_out.at[slot],
            dst_ref=pg_in.at[slot],
            send_sem=pg_send.at[slot],
            recv_sem=pg_recv.at[slot],
            device_id=at_z(z_out),
            device_id_type=MESH,
        )

    def gd_copy(b):
        return pltpu.make_async_remote_copy(
            src_ref=gd_out.at[b],
            dst_ref=gd_in.at[b],
            send_sem=gd_send.at[b],
            recv_sem=gd_recv.at[b],
            device_id=at_z(z_out),
            device_id_type=MESH,
        )

    @pl.loop(0, chunks)
    def _(chunk):
        plane_keep(chunk).wait()

        @pl.loop(1, COLS)
        def _(i):
            plane_copy(chunk, i).wait_recv()

        rows = mul(
            unpick[...], landed[chunk].astype(F32).reshape(ALL, WIDTH).astype(BF16)
        ).astype(BF16)
        for part in range(PARTS):
            start = part * 2 * UNIT
            kind, high = part // 2, part % 2
            at = slice(high * WIDTH, (high + 1) * WIDTH)
            own[z, core, chunk, kind, :, at] = rows[start : start + UNIT]
            other[chunk, kind, :, at] = rows[start + UNIT : start + 2 * UNIT]

        @pl.when(edge)
        def _():
            other_edge(chunk).start()
            chain_full(z, chunk, 0).start()
            hand_thin(z, chunk).start()

        @pl.when(inner)
        def _():
            other_inner(chunk).start()
            chain_full(z, chunk, 0).start()
            chain_thin(z, chunk, 1).start()
            hand_full(z, chunk).start()

    for load in loads[4:]:
        load.wait()

    hidden_units = wup.shape[1]

    def pair(slot, chunk, kind, high):
        at = slice(high * WIDTH, (high + 1) * WIDTH)
        return jnp.concatenate(
            [own[slot, 0, chunk, kind, :, at], own[slot, 1, chunk, kind, :, at]], axis=0
        )

    def places():
        for chunk in range(chunks):
            for high in range(2):
                yield chunk, high, high * half_width + chunk * WIDTH

    def terms_inner(slot):
        @pl.loop(0, chunks)
        def _(chunk):
            hand_full(slot, chunk).wait_recv()

        preact = jnp.zeros((2 * UNIT, 2 * hidden_units), F32)
        back = jnp.zeros((2 * UNIT, 2 * hidden_units), F32)
        for chunk, high, at in places():
            here = slice(at, at + WIDTH)
            preact += mul(
                pair(slot, chunk, 0, high),
                jnp.concatenate([wup[here, :], wup_ward[here, :]], axis=1),
            )
            back += mul_t(
                pair(slot, chunk, 1, high),
                jnp.concatenate([wdn[:, here], wdn_ward[:, here]], axis=0),
            )
        squash = jax.nn.sigmoid(preact)
        hidden = preact * squash
        pre_grad = (back * (squash * (1.0 + preact * (1.0 - squash)))).astype(BF16)
        pg_out[slot] = pre_grad[:, hidden_units:]
        hidden = hidden.astype(BF16).astype(F32).T.astype(BF16)
        pre_grad = pre_grad[:, :hidden_units].astype(F32).T.astype(BF16)
        pg_copy(slot).start()
        for chunk, high, at in places():
            here = slice(at, at + WIDTH)
            gdn[:, here] += mul(hidden, pair(slot, chunk, 1, high))
            gup[:, here] += mul(pre_grad, pair(slot, chunk, 0, high))

    def terms_edge(slot):
        @pl.loop(0, chunks)
        def _(chunk):
            hand_thin(slot, chunk).wait_recv()

        pg_copy(slot).wait_recv()
        pre_grad = pg_in[slot].astype(F32).T.astype(BF16)
        for chunk, high, at in places():
            gup[:, at : at + WIDTH] += mul(pre_grad, pair(slot, chunk, 0, high))

    def toward_out(far):
        return lax.rem(z + RING + out_sign * far, RING)

    def relay_out(far, chunk):
        slot = toward_out(far)
        chain_full(slot, chunk, 0).wait_recv()
        chain_full(slot, chunk, 0).start()

        @pl.when(edge)
        def _():
            hand_thin(slot, chunk).start()

        @pl.when(inner)
        def _():
            hand_full(slot, chunk).start()

    def relay_in(far, chunk):
        slot = toward_out(-far)
        chain_full(slot, chunk, 0).wait_recv()
        chain_thin(slot, chunk, 0).start()
        hand_full(slot, chunk).start()

    def edge_unit(i):
        thin = (i == 0) | (lax.rem(i, 2) == 1)
        far = jnp.where(i == 0, 1, (i + 3) // 2)
        return thin, toward_out(jnp.where(thin, -far, i // 2 - 1))

    @pl.when(edge)
    def _():
        @pl.loop(0, chunks)
        def _(chunk):
            other_inner(chunk).wait_recv()
            transit_edge(chunk).start()
            relay_out(1, chunk)

        @pl.loop(0, chunks)
        def _(chunk):
            relay_out(2, chunk)

        @pl.loop(0, RING)
        def _(i):
            thin, slot = edge_unit(i)

            @pl.when(thin)
            def _():
                @pl.loop(0, chunks)
                def _(chunk):
                    chain_thin(slot, chunk, 0).wait_recv()
                    hand_thin(slot, chunk).start()

            terms_edge(slot)

    @pl.when(inner)
    def _():
        @pl.loop(0, chunks)
        def _(chunk):
            relay_in(1, chunk)

        for i in range(2):
            ward_weights(i).wait_recv()

        def relay_in_at(item):
            relay_in(item // chunks + 1, lax.rem(item, chunks))

        steps = (HALF - 1) * chunks

        @pl.loop(0, steps)
        def _(item):
            relay_out(item // chunks + 1, lax.rem(item, chunks))

            @pl.when(item >= LAG)
            def _():
                relay_in_at(item + chunks - LAG)

            @pl.when(lax.rem(item, 3) == 2)
            def _():
                turn = item // 3
                terms_inner(
                    toward_out(jnp.where(lax.rem(turn, 2) == 0, turn // 2, -((turn + 1) // 2)))
                )

        @pl.loop(0, LAG)
        def _(i):
            relay_in_at(steps + chunks - LAG + i)

        terms_inner(toward_out(-HALF))

        span = gd_out.shape[2]
        for b in range(gd_out.shape[0]):
            gd_out[b] = gdn[hidden_units:, b * span : (b + 1) * span].astype(BF16)
            gd_copy(b).start()

    model_width = tok.shape[1]
    block = 128
    leaves = jnp.broadcast_to(leaving_ref[...], (block, block)) == ex
    ring_at, line_at = (cx, cy), (cy, cx)
    middle = SIDE

    def tile_home(axis, ring_to, line_to):
        to = line_to * SIDE + ring_to if axis == 0 else ring_to * SIDE + line_to
        return (dp, to * 2 + zhi)

    def ring_next(axis, far):
        return lax.rem(ring_at[axis] + far, SIDE)

    def ring_to(axis, side):
        return tile_home(axis, ring_next(axis, 1 if side == 0 else SIDE - 1), line_at[axis])

    def part_of(side):
        return pl.ds(0, middle) if side == 0 else pl.ds(middle, middle)

    def hop_copy(axis, side):
        return pltpu.make_async_remote_copy(
            src_ref=tiles.at[axis, ring_next(axis, 2), part_of(side)],
            dst_ref=hop.at[axis, side],
            send_sem=hop_send.at[axis, side],
            recv_sem=hop_recv.at[axis, side],
            device_id=ring_to(axis, side),
            device_id_type=MESH,
        )

    def ring_copy(axis, side, late):
        part = part_of(side if late else 1 - side)
        return pltpu.make_async_remote_copy(
            src_ref=tiles.at[axis, ring_next(axis, 1 if side == 0 else SIDE - 1), part],
            dst_ref=got.at[axis, side, part],
            send_sem=ring_send.at[axis, side, late],
            recv_sem=ring_recv.at[axis, side, late],
            device_id=ring_to(axis, side),
            device_id_type=MESH,
        )

    def fin_copy(axis, far):
        line_to = lax.rem(line_at[axis] + far, SIDE)
        return pltpu.make_async_remote_copy(
            src_ref=summed.at[axis, pl.ds(line_to * 2, 2)],
            dst_ref=fin.at[axis, far - 1],
            send_sem=fin_send.at[axis, far - 1],
            recv_sem=fin_recv.at[axis, far - 1],
            device_id=tile_home(axis, ring_at[axis], line_to),
            device_id_type=MESH,
        )

    def last_copy(axis):
        return pltpu.make_async_remote_copy(
            src_ref=summed.at[axis, line_at[axis] * 2 + me_other],
            dst_ref=last.at[axis],
            send_sem=last_send.at[axis],
            recv_sem=last_recv.at[axis],
            device_id=twin,
            device_id_type=MESH,
        )

    def sort_tiles(axis, leave):
        rows = tiles.shape[3]
        for tile in range(2 * COLS):
            by_tile[tile] = leave[tile * rows : (tile + 1) * rows, :]

        @pl.loop(0, 2 * COLS)
        def _(owner):
            to = owner // 2
            ty, tx = to // SIDE, lax.rem(to, SIDE)
            r, l = (tx, ty) if axis == 0 else (ty, tx)
            tiles[axis, r, l * 2 + lax.rem(owner, 2)] = by_tile[adopt_ref[owner]]

        for side in range(2):
            hop_copy(axis, side).start()
        for side in range(2):
            ring_copy(axis, side, 0).start()

    @pl.loop(0, model_width // block)
    def _(b):
        at = pl.ds(pl.multiple_of(b * block, block), block)
        step = adam_step(gup[:, at].T, mup[at, :], vup[at, :])
        sup[at, :] = step.astype(BF16)
        leave_up[at, :] = jnp.where(leaves, step, 0.0).astype(BF16)

    sort_tiles(0, leave_up)

    def pass_on(axis):
        for side in range(2):
            hop_copy(axis, side).wait_recv()
            to = ring_next(axis, 1 if side == 0 else SIDE - 1)
            part = part_of(side)
            tiles[axis, to, part] = tiles[axis, to, part] + hop[axis, side]
            ring_copy(axis, side, 1).start()

    span = gd_in.shape[2]

    @pl.loop(0, gd_in.shape[0])
    def _(b):
        @pl.when(edge)
        def _():
            gd_copy(b).wait_recv()
            gdn[0:hidden_units, pl.ds(pl.multiple_of(b * span, block), span)] = gd_in[b].astype(F32)

        @pl.loop(0, span // block)
        def _(i):
            at = pl.ds(pl.multiple_of(b * span + i * block, block), block)
            step = adam_step(gdn[0:hidden_units, at], mdn[:, at], vdn[:, at])
            sdn[:, at] = step.astype(BF16)
            leave_dn[at, :] = jnp.where(leaves, step, 0.0).T.astype(BF16)

    pass_on(0)
    sort_tiles(1, leave_dn)

    pass_on(1)

    for axis in range(2):
        for side in range(2):
            for late in range(2):
                ring_copy(axis, side, late).wait_recv()
        summed[axis] = tiles[axis, ring_at[axis]] + got[axis, 0] + got[axis, 1]
        for far in range(1, SIDE):
            fin_copy(axis, far).start()

    for axis in range(2):
        for far in range(1, SIDE):
            fin_copy(axis, far).wait_recv()
        mine = pl.ds(line_at[axis] * 2, 2)
        summed[axis, mine] = summed[axis, mine] + fin[axis, 0] + fin[axis, 1] + fin[axis, 2]
        last_copy(axis).start()

    for axis in range(2):
        last_copy(axis).wait_recv()
        adopted_ref[axis] = summed[axis, line_at[axis] * 2 + zhi] + last[axis]

    for axis in range(2):
        for side in range(2):
            hop_copy(axis, side).wait_send()
            for late in range(2):
                ring_copy(axis, side, late).wait_send()
        for far in range(1, SIDE):
            fin_copy(axis, far).wait_send()
        last_copy(axis).wait_send()

    @pl.loop(0, chunks)
    def _(chunk):
        @pl.loop(1, COLS)
        def _(i):
            plane_copy(chunk, i).wait_send()

        other_inner(chunk).wait_send()
        chain_full(z, chunk, 0).wait_send()

        @pl.when(edge)
        def _():
            transit_edge(chunk).wait_send()
            hand_thin(z, chunk).wait_send()

            @pl.loop(1, 3)
            def _(far):
                chain_full(toward_out(far), chunk, 0).wait_send()
                hand_thin(toward_out(far), chunk).wait_send()

            @pl.loop(1, 6)
            def _(far):
                hand_thin(toward_out(-far), chunk).wait_send()

        @pl.when(inner)
        def _():
            chain_thin(z, chunk, 1).wait_send()
            hand_full(z, chunk).wait_send()

            @pl.loop(1, 4)
            def _(far):
                chain_full(toward_out(far), chunk, 0).wait_send()
                hand_full(toward_out(far), chunk).wait_send()

            @pl.loop(1, 5)
            def _(far):
                chain_thin(toward_out(-far), chunk, 0).wait_send()
                hand_full(toward_out(-far), chunk).wait_send()

    @pl.when(edge)
    def _():
        for i in range(2):
            ward_weights(i).wait_send()

    @pl.when(inner)
    def _():
        @pl.loop(0, RING)
        def _(slot):
            pg_copy(slot).wait_send()

        @pl.loop(0, gd_out.shape[0])
        def _(b):
            gd_copy(b).wait_send()


def expert_steps(leaving, tile_owner, routes, gates, tokens, cotangent, w_up, w_down, m_up, v_up, m_down, v_down):
    count, model_width = tokens.shape
    hidden = w_up.shape[1]
    chunks = model_width // 2 // WIDTH
    tile_rows = model_width // tile_owner.shape[0]
    smem = pl.BlockSpec(memory_space=pltpu.SMEM)
    vmem = pl.BlockSpec(memory_space=pltpu.VMEM)
    anyw = pl.BlockSpec(memory_space=pl.ANY)
    dma = pltpu.SemaphoreType.DMA
    return pl.pallas_call(
        kernel,
        out_shape=(
            jax.ShapeDtypeStruct((model_width, hidden), BF16),
            jax.ShapeDtypeStruct((hidden, model_width), BF16),
            jax.ShapeDtypeStruct((2, tile_rows, hidden), BF16),
        ),
        in_specs=[vmem, smem, vmem, vmem] + [anyw] * 8,
        out_specs=(vmem, vmem, vmem),
        scratch_shapes=[
            pltpu.VMEM((count, model_width), BF16),
            pltpu.VMEM((count, model_width), BF16),
            pltpu.VMEM((model_width, hidden), BF16),
            pltpu.VMEM((hidden, model_width), BF16),
            pltpu.VMEM((model_width, hidden), BF16),
            pltpu.VMEM((hidden, model_width), BF16),
            pltpu.VMEM((model_width, hidden), BF16),
            pltpu.VMEM((model_width, hidden), BF16),
            pltpu.VMEM((hidden, model_width), BF16),
            pltpu.VMEM((hidden, model_width), BF16),
            pltpu.VMEM((ALL, PARTS * count), BF16),
            pltpu.VMEM((PARTS * 2 * UNIT, ALL), BF16),
            pltpu.VMEM((chunks, COLS, MSG, WIDTH), BF16),
            pltpu.VMEM((chunks, COLS, MSG, WIDTH), BF16),
            pltpu.VMEM((RING, 2, chunks, 2, UNIT, 2 * WIDTH), BF16),
            pltpu.VMEM((chunks, 2, UNIT, 2 * WIDTH), BF16),
            pltpu.VMEM((chunks, 2, UNIT, 2 * WIDTH), BF16),
            pltpu.VMEM((hidden, model_width), F32),
            pltpu.VMEM((2 * hidden, model_width), F32),
            pltpu.VMEM((RING, 2 * UNIT, hidden), BF16),
            pltpu.VMEM((RING, 2 * UNIT, hidden), BF16),
            pltpu.VMEM((7, hidden, model_width // 7), BF16),
            pltpu.VMEM((7, hidden, model_width // 7), BF16),
            pltpu.SMEM((2 * COLS,), jnp.int32),
            pltpu.VMEM((model_width, hidden), BF16),
            pltpu.VMEM((model_width, hidden), BF16),
            pltpu.VMEM((2 * COLS, tile_rows, hidden), BF16),
            pltpu.VMEM((2, SIDE, 2 * SIDE, tile_rows, hidden), BF16),
            pltpu.VMEM((2, 2, SIDE, tile_rows, hidden), BF16),
            pltpu.VMEM((2, 2, 2 * SIDE, tile_rows, hidden), BF16),
            pltpu.VMEM((2, 2 * SIDE, tile_rows, hidden), BF16),
            pltpu.VMEM((2, SIDE - 1, 2, tile_rows, hidden), BF16),
            pltpu.VMEM((2, tile_rows, hidden), BF16),
            dma((8,)),
            dma((chunks, COLS)),
            dma((chunks, COLS)),
            dma((chunks,)),
            dma((2, RING, chunks)),
            dma((RING, chunks)),
            dma((chunks,)),
            dma((chunks,)),
            dma((chunks,)),
            dma((RING, chunks)),
            dma((RING, chunks)),
            dma((2,)),
            dma((2,)),
            dma((RING,)),
            dma((RING,)),
            dma((7,)),
            dma((7,)),
            dma((2, 2)),
            dma((2, 2)),
            dma((2, 2, 2)),
            dma((2, 2, 2)),
            dma((2, SIDE - 1)),
            dma((2, SIDE - 1)),
            dma((2,)),
            dma((2,)),
        ],
        compiler_params=pltpu.CompilerParams(
            collective_id=0, has_side_effects=True, vmem_limit_bytes=52 * 1024 * 1024
        ),
        name="expert_steps",
    )(leaving, tile_owner, routes, gates, tokens, cotangent, w_up, w_down, m_up, v_up, m_down, v_down)


def on_device(
    tokens, cotangent, gates, routes, w_up, w_down, m_up, v_up, m_down, v_down, leaving, tile_owner
):
    tok_count = tokens.shape[0]
    step_up, step_down, adopted = expert_steps(
        leaving.reshape(1, 1),
        tile_owner,
        routes.reshape(1, tok_count),
        gates.reshape(1, tok_count),
        tokens,
        cotangent,
        w_up[0],
        w_down[0],
        m_up[0],
        v_up[0],
        m_down[0],
        v_down[0],
    )
    keep_own = lax.axis_index("expert") != leaving[0]
    update_up = jnp.where(keep_own, step_up, jnp.zeros_like(step_up))[None]
    update_down = jnp.where(keep_own, step_down, jnp.zeros_like(step_down))[None]
    return (update_up, update_down, adopted[0][None], adopted[1][None])


def solution(mesh):
    placed = (
        P(("dp", "expert"), None),
        P(("dp", "expert"), None),
        P(("dp", "expert"), None),
        P(("dp", "expert"), None),
        P("expert", None, "dp"),
        P("expert", "dp", None),
        P("expert", None, "dp"),
        P("expert", None, "dp"),
        P("expert", "dp", None),
        P("expert", "dp", None),
        P(),
        P(),
    )
    return jax.shard_map(
        on_device,
        mesh=mesh,
        in_specs=placed,
        out_specs=(
            P("expert", None, "dp"),
            P("expert", "dp", None),
            P("expert", None, "dp"),
            P("expert", None, "dp"),
        ),
        check_vma=False,
    )
```
